32 devices in a mesh: mesh: 8 (over z, y), member: 4 (over x, core).
Axes of the slice: x: 2, y: 2, z: 4, core: 2. Of those that a mesh axis runs over, the one named last changes fastest.
Arguments:
- node_states: bfloat16 [8, 4096, 512], P('member', 'mesh'), may hold values from -60 to 60
- projection: bfloat16 [512, 1536], P('member'), may hold values from -12 to 12
- output_weight: bfloat16 [512, 512], P('member'), may hold values from -0.25 to 0.25
- up_weight: bfloat16 [512, 2048], P('member'), may hold values from -0.25 to 0.25
- down_weight: bfloat16 [2048, 512], P('member'), may hold values from -0.125 to 0.125
- attention_gain: float32 [512], replicated, may hold values from 0.5 to 2
- feedforward_gain: float32 [512], replicated, may hold values from 0.5 to 2
- tile_lists: int32 [32, 8], P('mesh'), may hold values from 0 to 31, as said below
- tile_counts: int32 [32], P('mesh'), may hold values from 4 to 8, as said below
Outputs:
- updated_states: bfloat16 [8, 4096, 512], P('member', 'mesh')
The draws below stay inside these ranges and needn't reach their ends.
Inputs may be any that keep to these rules, and one draw needn't show every extreme that they name: `tile_lists`: entry 0 of tile t's list is t. Every entry names a tile of the device that holds t, or one of the last 4 tiles of the device before it, or one of the first 4 tiles of the device after it along mesh (the first and last devices are neighbours). The first tile_counts[t] entries are distinct; later entries are ignored. `tile_counts`: every device holds a tile whose count is 8.
All inputs are finite; a program needn't handle non-finite values.
Results may differ from the reference program's by a relative error of at most 0.0056.
Values may be sent and summed in bfloat16 or wider, within the bound.
No kernel may reach another device: no remote copies, remote signals or barrier semaphores. Data moves between devices by JAX's collectives and lax.ppermute only.
A program may use at most 128 MiB of HBM per device.

```python
import math
import jax
import jax.numpy as jnp
from jax import lax

D = 512
HEADS = 4
FF = 2048
TILE = 128
TILES_DEV = 4
RIM_T = 4
KT = 8
MEMBERS = 8
TILES = 32
NODES = 4096


def draw_node_states(key, part):
    sample = jax.random.normal(key, (MEMBERS, NODES, D), jnp.float32)
    return jnp.clip(sample, -60.0, 60.0).astype(jnp.bfloat16)


def draw_projection(key, part):
    sample = jnp.clip(jax.random.normal(key, (D, 3 * D), jnp.float32), -6.0, 6.0) * D ** (-0.5)
    return jnp.clip(sample, -12.0, 12.0).astype(jnp.bfloat16)


def tile_plan(key):
    sample = jax.random.fold_in(key, 7)
    devices = TILES // TILES_DEV
    window_tiles = TILES_DEV + 2 * RIM_T
    tile_ids = jnp.arange(TILES, dtype=jnp.int32)
    owner = tile_ids // TILES_DEV
    inner = tile_ids % TILES_DEV
    tile_keys = jax.random.split(sample, TILES)

    def pick(tile_key, own):
        shuffled = jax.random.permutation(tile_key, window_tiles - 1).astype(jnp.int32)
        shuffled = jnp.where(shuffled >= own, shuffled + 1, shuffled)
        return jnp.concatenate([own[None], shuffled[:KT - 1]])
    entries = jax.vmap(pick)(tile_keys, inner + RIM_T)
    owner_col = owner[:, None]
    leading = jnp.mod(owner_col - 1, devices) * TILES_DEV + TILES_DEV - RIM_T + entries
    middle = owner_col * TILES_DEV + entries - RIM_T
    trailing = jnp.mod(owner_col + 1, devices) * TILES_DEV + entries - RIM_T - TILES_DEV
    global_ids = jnp.where(entries < RIM_T, leading, jnp.where(entries < RIM_T + TILES_DEV, middle, trailing))
    counts = jax.random.randint(jax.random.fold_in(sample, 1), (TILES,), (KT + 1) // 2, KT + 1).astype(jnp.int32)
    counts = jnp.where(inner == 0, KT, counts).astype(jnp.int32)
    column = jnp.arange(KT, dtype=jnp.int32)
    global_ids = jnp.where(column[None, :] < counts[:, None], global_ids, tile_ids[:, None])
    return (global_ids.astype(jnp.int32), counts)


def draw_tile_lists(key, part):
    return tile_plan(key)[0]


def draw_tile_counts(key, part):
    return tile_plan(key)[1]


def steps_of(own_key, shape, cuts, low, largest):
    level, own = 1.0, jax.random.fold_in(own_key, 6)
    for axis_at, blocks in cuts:
        steps = jnp.exp(jax.random.uniform(jax.random.fold_in(own, axis_at), (blocks,), jnp.float32, low / len(cuts), largest / len(cuts)))
        level = level * jnp.repeat(steps, shape[axis_at] // blocks).reshape([-1 if axis == axis_at else 1 for axis in range(len(shape))])
    return level


def normal_values(rng, shape, scale, reach, pieces=(), kind=jnp.bfloat16):
    loudness = steps_of(rng, shape, pieces, -0.22, 0.18) if pieces else 1.0
    result = jax.random.normal(rng, shape, jnp.float32) * scale * loudness
    return jnp.minimum(jnp.maximum(result, -reach), reach).astype(kind)


def setup_inputs(seed: int = 0) -> dict:
    key_list = jax.random.split(jax.random.key(seed), 10)
    return {
        "node_states": draw_node_states(jax.random.fold_in(key_list[9], 71), 0),
        "projection": draw_projection(jax.random.fold_in(key_list[9], 71), 0),
        "output_weight": normal_values(key_list[2], (D, D), D ** -0.5, 0.25, ((0, 4),)),
        "up_weight": normal_values(key_list[3], (D, FF), D ** -0.5, 0.25, ((0, 4),)),
        "down_weight": normal_values(key_list[4], (FF, D), FF ** -0.5, 0.125, ((0, 4),)),
        "attention_gain": jnp.clip(jnp.exp(jax.random.uniform(key_list[5], (D,), jnp.float32, math.log(0.5), math.log(2.0))), 0.5, 2.0),
        "feedforward_gain": jnp.clip(jnp.exp(jax.random.uniform(key_list[6], (D,), jnp.float32, math.log(0.5), math.log(2.0))), 0.5, 2.0),
        "tile_lists": draw_tile_lists(jax.random.fold_in(key_list[9], 71), 0),
        "tile_counts": draw_tile_counts(jax.random.fold_in(key_list[9], 71), 0),
    }


def layer_norm(node_rows, gain):
    values = node_rows.astype(jnp.float32)
    center = values - lax.optimization_barrier(jnp.mean(values, axis=-1, keepdims=True))
    spread = lax.optimization_barrier(jnp.mean(center * center, axis=-1, keepdims=True))
    return (center * lax.rsqrt(spread + 1e-05) * gain).astype(jnp.bfloat16)

def attend(queries, window, tile_ids, counts):
    members, groups, tile_rows, model_width = queries.shape
    entries = tile_ids.shape[1]
    head_size = model_width // HEADS
    picked = jnp.take(window, tile_ids.reshape(-1), axis=1)
    picked = picked.reshape(members, groups, entries * tile_rows, 2 * model_width)
    key_part = picked[..., :model_width].reshape(members, groups, entries * tile_rows, HEADS, head_size).astype(jnp.float32)
    value_part = picked[..., model_width:].reshape(members, groups, entries * tile_rows, HEADS, head_size).astype(jnp.float32)
    query_part = queries.reshape(members, groups, tile_rows, HEADS, head_size).astype(jnp.float32)
    scores = jnp.einsum('mgqhe,mgkhe->mghqk', query_part, key_part) / math.sqrt(head_size)
    usable = (jnp.arange(entries * tile_rows) // tile_rows)[None, :] < counts[:, None]
    scores = jnp.where(usable[None, :, None, None, :], scores, -jnp.inf)
    highest = lax.optimization_barrier(jnp.max(scores, axis=-1, keepdims=True))
    weights = jnp.exp(scores - highest)
    summed = lax.optimization_barrier(jnp.sum(weights, axis=-1, keepdims=True))
    rounded = lax.optimization_barrier(weights.astype(jnp.bfloat16)).astype(jnp.float32)
    blended = jnp.einsum('mghqk,mgkhe->mghqe', rounded, value_part) / summed
    blended = jnp.transpose(blended, (0, 1, 3, 2, 4)).reshape(members, groups, tile_rows, model_width)
    return blended.astype(jnp.bfloat16)

def reference(node_states, projection, output_weight, up_weight, down_weight, attention_gain, feedforward_gain, tile_lists, tile_counts):
    members, node_count, model_width = node_states.shape
    normed = layer_norm(node_states, attention_gain)

    def project(node_rows):
        projected = jnp.dot(node_rows, projection, preferred_element_type=jnp.float32)
        return (projected[:, :model_width].astype(jnp.bfloat16), projected[:, model_width:].astype(jnp.bfloat16))
    queries, pairs = lax.map(project, normed)
    window = pairs.reshape(members, TILES, TILE, 2 * model_width)
    grouped = jnp.transpose(queries.reshape(members, TILES // 2, 2, TILE, model_width), (1, 0, 2, 3, 4))
    lists_grouped = tile_lists.reshape(TILES // 2, 2, KT)
    counts_grouped = tile_counts.reshape(TILES // 2, 2)

    def one_group(element):
        return attend(element[0], window, element[1], element[2])
    attended = lax.map(one_group, (grouped, lists_grouped, counts_grouped))
    attended = jnp.transpose(attended, (1, 0, 2, 3, 4)).reshape(members, node_count, model_width)

    def finish(element):
        states, blended = element
        middle = (states.astype(jnp.float32) + jnp.dot(blended, output_weight, preferred_element_type=jnp.float32)).astype(jnp.bfloat16)
        middle = lax.optimization_barrier(middle)
        normed_second = layer_norm(middle, feedforward_gain)
        hidden = jax.nn.gelu(jnp.dot(normed_second, up_weight, preferred_element_type=jnp.float32), approximate=True).astype(jnp.bfloat16)
        return (middle.astype(jnp.float32) + jnp.dot(hidden, down_weight, preferred_element_type=jnp.float32)).astype(jnp.bfloat16)
    return lax.map(finish, (node_states, attended))
```

```python
import functools
import math

import jax
import jax.numpy as jnp
from jax import lax
from jax.experimental import pallas as pl
from jax.experimental.pallas import tpu as pltpu
from jax.sharding import PartitionSpec as P

HEADS = 4
RIM_T = 4
SURE = 4
BF16 = jnp.bfloat16
F32 = jnp.float32
VMEM = pltpu.VMEM
ANY = pl.ANY


def norm_rows(rows, gain):
    values = rows.astype(F32)
    center = values - jnp.mean(values, axis=-1, keepdims=True)
    spread = jnp.mean(center * center, axis=-1, keepdims=True)
    return (center * lax.rsqrt(spread + 1e-05) * gain).astype(BF16)


def dot(a, b):
    return lax.dot_general(a, b, (((1,), (0,)), ((), ())), preferred_element_type=F32)


def dot_t(a, b):
    return lax.dot_general(a, b, (((1,), (1,)), ((), ())), preferred_element_type=F32)


def copies(me, pieces, whole, sems, first):
    rows = pieces[0].shape[0]
    return [
        pltpu.make_async_copy(
            piece, whole.at[pl.ds(pl.multiple_of((me ^ k) * rows, rows), rows)], sems.at[first + k]
        )
        for k, piece in enumerate(pieces)
    ]


def attend_tiles(info, base, q_ref, kv_ref, out_ref, tiles, tile_rows, width, entries):
    head = width // HEADS
    scale = math.log2(math.e) / math.sqrt(head)
    stride = entries + 1

    def one_tile(t, carry):
        at = base + t * stride
        count = info[at + entries]
        starts = [
            pl.multiple_of(info[at + j] * tile_rows, tile_rows) for j in range(entries)
        ]
        row = pl.multiple_of(t * tile_rows, tile_rows)
        for h in range(HEADS):
            cols = slice(h * head, (h + 1) * head)
            vcols = slice(width + h * head, width + (h + 1) * head)
            q = q_ref[pl.ds(row, tile_rows), cols]
            keys = jnp.concatenate(
                [kv_ref[pl.ds(s, tile_rows), cols] for s in starts], axis=0
            )
            scores = dot_t(q, keys)
            parts = []
            for j in range(entries):
                part = scores[:, j * tile_rows : (j + 1) * tile_rows]
                if j >= SURE:
                    part = jnp.where(j < count, part, -jnp.inf)
                parts.append(part)
            scores = jnp.concatenate(parts, axis=1)
            highest = jnp.max(scores, axis=-1, keepdims=True)
            weights = jnp.exp2((scores - highest) * scale)
            total = jnp.sum(weights, axis=-1, keepdims=True)
            values = jnp.concatenate(
                [kv_ref[pl.ds(s, tile_rows), vcols] for s in starts], axis=0
            )
            blended = dot(weights.astype(BF16), values)
            out_ref[pl.ds(row, tile_rows), cols] = (blended / total).astype(BF16)
        return carry

    lax.fori_loop(0, tiles, one_tile, 0)


def near_body(info, keep, got, far, gain, *rest, n_pieces, tiles, tile_rows, entries):
    pieces, (attended, q_keep, kv_two, weight, kv, q_got, sems) = (
        rest[:n_pieces],
        rest[n_pieces:],
    )
    rows, width = keep.shape
    me = info[0]
    loads = copies(me, pieces, weight, sems, 0)
    for load in loads:
        load.start()
    for load in loads:
        load.wait()
    block = 256
    for at, (source, queries) in enumerate(((keep, q_keep), (got, q_got), (far, None))):

        def one_block(b, carry, at=at, source=source, queries=queries):
            row = pl.multiple_of(b * block, block)
            normed = norm_rows(source[pl.ds(row, block), :], gain[...])
            if queries is not None:
                queries[pl.ds(row, block), :] = dot(normed, weight[:, :width]).astype(BF16)
            pairs = dot(normed, weight[:, width:]).astype(BF16)
            kv[pl.ds(at * rows + row, block), :] = pairs
            if queries is not None:
                kv_two[pl.ds(at * rows + row, block), :] = pairs
            return carry

        lax.fori_loop(0, rows // block, one_block, 0)
    attend_tiles(info, 1, q_got, kv, attended, tiles, tile_rows, width, entries)


def far_body(
    info, states, far, q_keep, kv_two, gain, second_gain, *rest,
    n_pieces, tiles, tile_rows, entries,
):
    proj, outs, ups = (rest[i * n_pieces : (i + 1) * n_pieces] for i in range(3))
    middle, hidden, weight, out_weight, up_weight, kv, attended, sems = rest[3 * n_pieces :]
    rows, width = far.shape
    me = info[0]
    loads = (
        copies(me, proj, weight, sems, 0)
        + copies(me, outs, out_weight, sems, n_pieces)
        + copies(me, ups, up_weight, sems, 2 * n_pieces)
    )
    both = pltpu.make_async_copy(
        kv_two, kv.at[pl.ds(0, 2 * rows)], sems.at[3 * n_pieces]
    )
    both.start()
    for load in loads:
        load.start()
    for load in loads[:n_pieces]:
        load.wait()
    block = 256

    def one_block(b, carry):
        row = pl.multiple_of(b * block, block)
        normed = norm_rows(far[pl.ds(row, block), :], gain[...])
        kv[pl.ds(2 * rows + row, block), :] = dot(normed, weight[:, width:]).astype(BF16)
        return carry

    lax.fori_loop(0, rows // block, one_block, 0)
    both.wait()
    attend_tiles(info, 1, q_keep, kv, attended, tiles, tile_rows, width, entries)
    for load in loads[n_pieces:]:
        load.wait()
    widen_rows(states, attended, out_weight, up_weight, second_gain, middle, hidden)


def gelu(x):
    return jax.nn.gelu(x, approximate=True)


def widen_rows(states, attended, out_weight, up_weight, gain, middle, hidden):
    block = 256
    rows = attended.shape[0]

    def one_block(b, carry):
        at = pl.ds(pl.multiple_of(b * block, block), block)
        mid = (states[at, :].astype(F32) + dot(attended[at, :], out_weight[...])).astype(BF16)
        middle[at, :] = mid
        normed = norm_rows(mid, gain[...])
        hidden[at, :] = gelu(dot(normed, up_weight[...])).astype(BF16)
        return carry

    lax.fori_loop(0, rows // block, one_block, 0)


def back_body(info, states, attended, second_gain, *rest, n_pieces):
    outs, ups = (rest[i * n_pieces : (i + 1) * n_pieces] for i in range(2))
    middle, hidden, out_weight, up_weight, sems = rest[2 * n_pieces :]
    me = info[0]
    loads = copies(me, outs, out_weight, sems, 0) + copies(me, ups, up_weight, sems, n_pieces)
    for load in loads:
        load.start()
    for load in loads:
        load.wait()
    widen_rows(states, attended, out_weight, up_weight, second_gain, middle, hidden)


def down_body(info, middle_k, hidden_k, middle_g, hidden_g, *rest, n_pieces):
    pieces, (out, weight, sems) = rest[:n_pieces], rest[n_pieces:]
    me, mine = info[0], info[1]
    loads = copies(me, pieces, weight, sems, 0)
    for load in loads:
        load.start()
    for load in loads:
        load.wait()
    block = 256
    rows = middle_k.shape[0]
    for member, middle, hidden in ((mine, middle_k, hidden_k), (1 - mine, middle_g, hidden_g)):

        def one_block(b, carry, member=member, middle=middle, hidden=hidden):
            at = pl.ds(pl.multiple_of(b * block, block), block)
            out[member, at, :] = (
                middle[at, :].astype(F32) + dot(hidden[at, :], weight[...])
            ).astype(BF16)
            return carry

        lax.fori_loop(0, rows // block, one_block, 0)


def call(body, name, out_shapes, scratch, operands, spaces, flops, **static):
    specs = [pl.BlockSpec(memory_space=space) for space in spaces]
    outs = [jax.ShapeDtypeStruct(shape, BF16) for shape in out_shapes]
    return pl.pallas_call(
        functools.partial(body, **static),
        out_shape=outs,
        in_specs=specs,
        out_specs=[pl.BlockSpec(memory_space=VMEM) for _ in outs],
        scratch_shapes=scratch,
        name=name,
        cost_estimate=pl.CostEstimate(flops=flops, bytes_accessed=4 << 20, transcendentals=0),
        compiler_params=pltpu.CompilerParams(vmem_limit_bytes=48 << 20),
    )(*operands)


def exchange(axis, count, bit):
    return functools.partial(
        lax.ppermute, axis_name=axis, perm=[(i, i ^ bit) for i in range(count)]
    )


def on_device(
    node_states, projection, output_weight, up_weight, down_weight,
    attention_gain, feedforward_gain, tile_lists, tile_counts,
):
    members, rows, width = node_states.shape
    tiles, entries = tile_lists.shape
    tile_rows = rows // tiles
    hidden = up_weight.shape[1]
    ring, n = lax.axis_size("mesh"), lax.axis_size("member")
    if members != 2 or ring % 2 or ring < 4 or n & (n - 1) or RIM_T > tiles:
        raise ValueError("unsupported mesh")
    place, me = lax.axis_index("mesh"), lax.axis_index("member")
    side = place % 2
    bits = [1 << b for b in reversed(range(n.bit_length() - 1))]

    def gather(shard):
        pieces = {0: shard}
        for bit in bits:
            for k, piece in list(pieces.items()):
                pieces[k ^ bit] = exchange("member", n, bit)(piece)
        return [pieces[k] for k in range(n)]

    keep = lax.dynamic_index_in_dim(node_states, side, 0, keepdims=False)
    give = lax.dynamic_index_in_dim(node_states, 1 - side, 0, keepdims=False)
    proj = gather(projection)
    got = exchange("mesh", ring, 1)(give)
    outward = [(i, (i + (2 if i % 2 else -2)) % ring) for i in range(ring)]
    inward = [(i, (i + (-2 if i % 2 else 2)) % ring) for i in range(ring)]
    far_near = lax.ppermute(keep, "mesh", outward)
    far_late = lax.ppermute(got, "mesh", inward)
    table = jnp.concatenate([tile_lists, tile_counts[:, None]], axis=1)
    other = exchange("mesh", ring, 1)(table)
    outs = gather(output_weight)
    ups = gather(up_weight)
    downs = gather(down_weight)

    def slots(plan):
        ids = plan[:, :entries]
        owner, inner = ids // tiles, ids % tiles
        block = jnp.where(owner == place, 0, jnp.where(owner == place ^ 1, 1, 2))
        filled = jnp.concatenate([block * tiles + inner, plan[:, entries:]], axis=1)
        return jnp.concatenate([me[None], filled.reshape(-1)]).astype(jnp.int32)

    gain = attention_gain.reshape(1, width)
    second = feedforward_gain.reshape(1, width)
    whole = lambda shards: (n * shards.shape[0], shards.shape[1])
    S = pltpu.SMEM
    shape_static = dict(n_pieces=n, tiles=tiles, tile_rows=tile_rows, entries=entries)
    attended_got, q_keep, kv_two = call(
        near_body, "near",
        [(rows, width), (rows, width), (2 * rows, 2 * width)],
        [
            pltpu.VMEM(whole(projection), BF16),
            pltpu.VMEM((3 * rows, 2 * width), BF16),
            pltpu.VMEM((rows, width), BF16),
            pltpu.SemaphoreType.DMA((n,)),
        ],
        [slots(other), keep, got, far_near, gain, *proj],
        [S, VMEM, VMEM, VMEM, VMEM] + [ANY] * n,
        4 << 30, **shape_static,
    )
    attended_back = exchange("mesh", ring, 1)(attended_got)
    middle_k, hidden_k = call(
        far_body, "far",
        [(rows, width), (rows, hidden)],
        [
            pltpu.VMEM(whole(projection), BF16),
            pltpu.VMEM(whole(output_weight), BF16),
            pltpu.VMEM(whole(up_weight), BF16),
            pltpu.VMEM((3 * rows, 2 * width), BF16),
            pltpu.VMEM((rows, width), BF16),
            pltpu.SemaphoreType.DMA((3 * n + 1,)),
        ],
        [slots(table), keep, far_late, q_keep, kv_two, gain, second, *proj, *outs, *ups],
        [S, VMEM, VMEM, VMEM, ANY, VMEM, VMEM] + [ANY] * (3 * n),
        4 << 30, **shape_static,
    )
    middle_g, hidden_g = call(
        back_body, "back",
        [(rows, width), (rows, hidden)],
        [
            pltpu.VMEM(whole(output_weight), BF16),
            pltpu.VMEM(whole(up_weight), BF16),
            pltpu.SemaphoreType.DMA((2 * n,)),
        ],
        [me[None], give, attended_back, second, *outs, *ups],
        [S, VMEM, VMEM, VMEM] + [ANY] * (2 * n),
        2 << 30, n_pieces=n,
    )
    (result,) = call(
        down_body, "down",
        [node_states.shape],
        [pltpu.VMEM(whole(down_weight), BF16), pltpu.SemaphoreType.DMA((n,))],
        [jnp.stack([me, side]), middle_k, hidden_k, middle_g, hidden_g, *downs],
        [S, VMEM, VMEM, VMEM, VMEM] + [ANY] * n,
        2 << 30, n_pieces=n,
    )
    return result


def solution(mesh):
    in_specs = (
        P("member", "mesh", None),
        P("member", None),
        P("member", None),
        P("member", None),
        P("member", None),
        P(),
        P(),
        P("mesh", None),
        P("mesh"),
    )
    return jax.shard_map(
        on_device, mesh=mesh, in_specs=in_specs,
        out_specs=P("member", "mesh", None), check_vma=False,
    )
```

```python
import functools
import math

import jax
import jax.numpy as jnp
from jax import lax
from jax.experimental import pallas as pl
from jax.experimental.pallas import tpu as pltpu
from jax.sharding import PartitionSpec as P

HEADS = 4
RIM_T = 4
SURE = 4
BF16 = jnp.bfloat16
F32 = jnp.float32
VMEM = pltpu.VMEM
SMEM = pltpu.SMEM
ANY = pl.ANY


def norm_rows(rows, gain):
    values = rows.astype(F32)
    center = values - jnp.mean(values, axis=-1, keepdims=True)
    spread = jnp.mean(center * center, axis=-1, keepdims=True)
    return (center * lax.rsqrt(spread + 1e-05) * gain).astype(BF16)


def dot(a, b):
    return lax.dot_general(a, b, (((1,), (0,)), ((), ())), preferred_element_type=F32)


def dot_t(a, b):
    return lax.dot_general(a, b, (((1,), (1,)), ((), ())), preferred_element_type=F32)


def gelu(x):
    return jax.nn.gelu(x, approximate=True)


def piece_copies(me, pieces, whole, sems, first, cols=None):
    rows = pieces[0].shape[0]
    return [
        pltpu.make_async_copy(
            piece if cols is None else piece.at[:, cols],
            whole.at[pl.ds(pl.multiple_of((me ^ k) * rows, rows), rows)],
            sems.at[first + k],
        )
        for k, piece in enumerate(pieces)
    ]


def start_all(copies):
    for copy in copies:
        copy.start()


def wait_all(copies):
    for copy in copies:
        copy.wait()


def project_pairs(normed, weight, key_cols, value_cols, keys, values, row, tile_rows):
    count = normed.shape[0]
    keys[pl.ds(row, count), :] = dot(normed, weight[:, key_cols]).astype(BF16)
    block = dot(normed, weight[:, value_cols]).astype(BF16)
    for t in range(count // tile_rows):
        values[row // tile_rows + t] = block[t * tile_rows : (t + 1) * tile_rows].T


def attend_tiles(lists, counts, slot, q_ref, k_ref, v_ref, out_ref, scores, tops, tile_rows):
    tiles, entries = lists.shape
    width = q_ref.shape[1]
    head = width // HEADS
    scale = math.log2(math.e) / math.sqrt(head)
    zero = jnp.zeros((tile_rows, head), BF16)

    def stage(t, p, at):
        row = pl.multiple_of(t * tile_rows, tile_rows)
        first = q_ref[pl.ds(row, tile_rows), 2 * p * head : (2 * p + 1) * head]
        second = q_ref[pl.ds(row, tile_rows), (2 * p + 1) * head : (2 * p + 2) * head]
        both = jnp.concatenate(
            [jnp.concatenate([first, zero], 1), jnp.concatenate([zero, second], 1)], 0
        )
        cols = slice(2 * p * head, (2 * p + 2) * head)
        keys = jnp.concatenate(
            [
                k_ref[pl.ds(pl.multiple_of(slot[t * entries + j] * tile_rows, tile_rows), tile_rows), cols]
                for j in range(entries)
            ],
            0,
        )
        product = dot_t(keys, both)
        scores[at] = product
        top = None
        for j in range(entries):
            part = product[j * tile_rows : (j + 1) * tile_rows]
            part = jnp.max(part.reshape(tile_rows // 8, 8, 2 * tile_rows), axis=0)
            if j >= SURE:
                part = jnp.where(j < counts[t], part, -jnp.inf)
            top = part if top is None else jnp.maximum(top, part)
        top = jnp.max(top, axis=0, keepdims=True) * scale
        tops[at] = jnp.broadcast_to(top, tops.shape[1:])

    def blend(t, p, at):
        row = pl.multiple_of(t * tile_rows, tile_rows)
        top = tops[at, 0:1]
        total, outs = None, [None, None]
        for pair in range(0, entries, 2):
            weights = []
            for j in (pair, pair + 1):
                highest = jnp.where(j < counts[t], top, jnp.inf) if j >= SURE else top
                weight = jnp.exp2(scores[at, j * tile_rows : (j + 1) * tile_rows] * scale - highest)
                part = jnp.sum(weight.reshape(tile_rows // 8, 8, 2 * tile_rows), axis=0)
                total = part if total is None else total + part
                weights.append(weight.astype(BF16))
            weights = jnp.concatenate(weights, 0)
            for a in range(2):
                h = 2 * p + a
                values = jnp.concatenate(
                    [
                        v_ref[slot[t * entries + j], h * head : (h + 1) * head, :]
                        for j in (pair, pair + 1)
                    ],
                    1,
                )
                out = dot(values, weights[:, a * tile_rows : (a + 1) * tile_rows])
                outs[a] = out if outs[a] is None else outs[a] + out
        total = jnp.sum(total, axis=0, keepdims=True)
        for a in range(2):
            h = 2 * p + a
            out = outs[a] / total[:, a * tile_rows : (a + 1) * tile_rows]
            out_ref[pl.ds(row, tile_rows), h * head : (h + 1) * head] = out.T.astype(BF16)

    pairs = HEADS // 2
    stage(0, 0, 0)

    def one_tile(t, carry):
        for p in range(pairs):
            last = p == pairs - 1
            following = jnp.minimum(t + 1, tiles - 1) if last else t
            stage(following, 0 if last else p + 1, (p + 1) % 2)
            blend(t, p, p % 2)
        return carry

    lax.fori_loop(0, tiles, one_tile, 0)


def fill_slots(info, lists, slot):
    tiles, entries = lists.shape
    place, other = info[1], info[2]
    for t in range(tiles):
        for j in range(entries):
            tile = lists[t, j]
            owner = lax.div(tile, jnp.int32(tiles))
            block = jnp.where(owner == place, 0, jnp.where(owner == other, 1, 2))
            slot[t * entries + j] = block * tiles + lax.rem(tile, jnp.int32(tiles))


def near_body(info, keep, got, gain, *rest, n_pieces, tile_rows):
    pieces, (q_keep, q_got, k_out, v_out, weight, normed, queries, keys, values, sems) = (
        rest[:n_pieces],
        rest[n_pieces:],
    )
    rows, width = keep.shape
    me = info[0]
    loads = piece_copies(me, pieces, weight, sems, 0)
    start_all(loads)
    block = 256
    for at, source in enumerate((keep, got)):
        for b in range(rows // block):
            normed[at * rows + b * block : at * rows + (b + 1) * block] = norm_rows(
                source[b * block : (b + 1) * block, :], gain[...]
            )
    wait_all(loads)
    writes = []
    tiles = rows // tile_rows
    for at in range(2):
        span = pl.ds(at * rows, rows)
        part = normed[span]
        queries[span] = dot(part, weight[:, :width]).astype(BF16)
        project_pairs(
            part, weight, slice(width, 2 * width), slice(2 * width, 3 * width),
            keys, values, at * rows, tile_rows,
        )
        slots = pl.ds(at * tiles, tiles)
        for i, (source, target, where) in enumerate(
            ((queries, None, span), (keys, k_out, span), (values, v_out, slots))
        ):
            place = (q_keep, q_got)[at] if target is None else target.at[where]
            copy = pltpu.make_async_copy(
                source.at[where], place, sems.at[n_pieces + 3 * at + i]
            )
            copy.start()
            writes.append(copy)
    wait_all(writes)


def third_block(info, far, gain, pieces, k_near, v_near, weight, keys, values, sems, tile_rows):
    rows, width = far.shape
    n = len(pieces)
    tiles = rows // tile_rows
    loads = piece_copies(info[0], pieces, weight, sems, 0, pl.ds(width, 2 * width))
    near = [
        pltpu.make_async_copy(k_near, keys.at[pl.ds(0, 2 * rows)], sems.at[n]),
        pltpu.make_async_copy(v_near, values.at[pl.ds(0, 2 * tiles)], sems.at[n + 1]),
    ]
    start_all(loads)
    start_all(near)
    normed = norm_rows(far[...], gain[...])
    wait_all(loads)
    project_pairs(
        normed, weight, slice(0, width), slice(width, 2 * width), keys, values, 2 * rows, tile_rows
    )
    wait_all(near)


def got_body(info, lists, counts, far, queries, k_near, v_near, gain, *rest, n_pieces, tile_rows):
    pieces, (attended, weight, keys, values, scores, tops, slot, sems) = (
        rest[:n_pieces],
        rest[n_pieces:],
    )
    fill_slots(info, lists, slot)
    third_block(
        info, far, gain, pieces, k_near, v_near, weight, keys, values, sems, tile_rows
    )
    attend_tiles(
        lists, counts, slot, queries, keys, values, attended, scores, tops, tile_rows
    )


def keep_body(
    info, lists, counts, states, far, queries, k_near, v_near, gain, second_gain, *rest,
    n_pieces, tile_rows,
):
    proj, outs, ups = (rest[i * n_pieces : (i + 1) * n_pieces] for i in range(3))
    (
        middle, hidden, weight, out_weight, up_weight, keys, values, attended, scores, tops,
        slot, sems,
    ) = rest[3 * n_pieces :]
    me = info[0]
    first = n_pieces + 2
    late = piece_copies(me, outs, out_weight, sems, first) + piece_copies(
        me, ups, up_weight, sems, first + n_pieces
    )
    fill_slots(info, lists, slot)
    third_block(info, far, gain, proj, k_near, v_near, weight, keys, values, sems, tile_rows)
    start_all(late)
    attend_tiles(
        lists, counts, slot, queries, keys, values, attended, scores, tops, tile_rows
    )
    wait_all(late)
    widen_rows(states, attended, out_weight, up_weight, second_gain, middle, hidden, ())


def widen_rows(states, attended, out_weight, up_weight, gain, middle, hidden, before_up):
    block = 256
    rows = attended.shape[0]
    for b in range(rows // block):
        at = slice(b * block, (b + 1) * block)
        mid = (states[at, :].astype(F32) + dot(attended[at, :], out_weight[...])).astype(BF16)
        middle[at, :] = mid
        normed = norm_rows(mid, gain[...])
        if b == 0:
            wait_all(before_up)
        hidden[at, :] = gelu(dot(normed, up_weight[...])).astype(BF16)


def back_body(info, states, attended, second_gain, *rest, n_pieces):
    outs, ups = (rest[i * n_pieces : (i + 1) * n_pieces] for i in range(2))
    middle, hidden, out_weight, up_weight, sems = rest[2 * n_pieces :]
    early = piece_copies(info[0], outs, out_weight, sems, 0)
    late = piece_copies(info[0], ups, up_weight, sems, n_pieces)
    start_all(early)
    start_all(late)
    wait_all(early)
    widen_rows(states, attended, out_weight, up_weight, second_gain, middle, hidden, late)


def down_body(info, middle_k, hidden_k, middle_g, hidden_g, *rest, n_pieces):
    pieces, (out, weight, acc, sems) = rest[:n_pieces], rest[n_pieces:]
    me, side = info[0], info[3]
    block = pieces[0].shape[0]
    loads = [
        pltpu.make_async_copy(piece, weight.at[k], sems.at[k]) for k, piece in enumerate(pieces)
    ]
    start_all(loads)
    for k, load in enumerate(loads):
        load.wait()
        cols = pl.ds(pl.multiple_of((me ^ k) * block, block), block)
        for i, (middle, hidden) in enumerate(((middle_k, hidden_k), (middle_g, hidden_g))):
            product = dot(hidden[:, cols], weight[k])
            if k == 0:
                acc[i] = middle[...].astype(F32) + product
            elif k < n_pieces - 1:
                acc[i] += product
            else:
                out[jnp.where(i == 0, side, 1 - side)] = (acc[i] + product).astype(BF16)


def call(body, outs, out_spaces, scratch, operands, spaces, flops, **static):
    return pl.pallas_call(
        functools.partial(body, **static),
        out_shape=[jax.ShapeDtypeStruct(shape, BF16) for shape in outs],
        in_specs=[pl.BlockSpec(memory_space=space) for space in spaces],
        out_specs=[pl.BlockSpec(memory_space=space) for space in out_spaces],
        scratch_shapes=scratch,
        cost_estimate=pl.CostEstimate(
            flops=flops, bytes_accessed=4 << 20, transcendentals=0
        ),
        compiler_params=pltpu.CompilerParams(vmem_limit_bytes=VMEM_LIMIT),
    )(*operands)


VMEM_LIMIT = 24 << 20


def send(axis, perm, array):
    return lax.ppermute(array, axis, perm)


def layer(
    node_states, projection, output_weight, up_weight, down_weight,
    attention_gain, feedforward_gain, tile_lists, tile_counts,
):
    members, rows, width = node_states.shape
    tiles, entries = tile_lists.shape
    tile_rows = rows // tiles
    hidden = up_weight.shape[1]
    ring, n = lax.axis_size("mesh"), lax.axis_size("member")
    if members != 2 or ring % 2 or ring < 4 or n & (n - 1) or RIM_T > tiles:
        raise ValueError("unsupported mesh")
    place, me = lax.axis_index("mesh"), lax.axis_index("member")
    side = place & 1
    info = jnp.stack([me, place, place ^ 1, side]).astype(jnp.int32)
    bits = [1 << b for b in reversed(range(n.bit_length() - 1))]
    swap = [(i, i ^ 1) for i in range(ring)]
    outward = [(i, (i + (2 if i % 2 else -2)) % ring) for i in range(ring)]
    inward = [(i, (i + (-2 if i % 2 else 2)) % ring) for i in range(ring)]

    def gather(shard):
        pieces = {0: shard}
        for bit in bits:
            perm = [(i, i ^ bit) for i in range(n)]
            for k, piece in list(pieces.items()):
                pieces[k ^ bit] = send("member", perm, piece)
        return [pieces[k] for k in range(n)]

    give = lax.dynamic_index_in_dim(node_states, 1 - side, 0, keepdims=False)
    keep = lax.dynamic_index_in_dim(node_states, side, 0, keepdims=False)
    their_lists = send("mesh", swap, tile_lists)
    their_counts = send("mesh", swap, tile_counts)
    got = send("mesh", swap, give)
    proj = gather(projection)
    far_near = send("mesh", outward, keep)
    far_late = send("mesh", inward, got)
    outs = gather(output_weight)
    ups = gather(up_weight)
    downs = gather(down_weight)

    gain = attention_gain.reshape(1, width)
    second = feedforward_gain.reshape(1, width)
    whole = lambda shard, cols: pltpu.VMEM((n * shard.shape[0], cols), BF16)
    window = [
        pltpu.VMEM((3 * rows, width), BF16),
        pltpu.VMEM((3 * tiles, width, tile_rows), BF16),
    ]
    flash = [
        pltpu.VMEM((2, entries * tile_rows, 2 * tile_rows), F32),
        pltpu.VMEM((2, 8, 2 * tile_rows), F32),
        pltpu.SMEM((tiles * entries,), jnp.int32),
    ]
    sems = pltpu.SemaphoreType.DMA
    static = dict(n_pieces=n, tile_rows=tile_rows)
    q_keep, q_got, k_near, v_near = call(
        near_body,
        [(rows, width), (rows, width), (2 * rows, width), (2 * tiles, width, tile_rows)],
        [ANY, ANY, ANY, ANY],
        [
            whole(projection, 3 * width),
            pltpu.VMEM((2 * rows, width), BF16),
            pltpu.VMEM((2 * rows, width), BF16),
            pltpu.VMEM((2 * rows, width), BF16),
            pltpu.VMEM((2 * tiles, width, tile_rows), BF16),
            sems((n + 6,)),
        ],
        [info, keep, got, gain, *proj],
        [SMEM, VMEM, VMEM, VMEM] + [ANY] * n,
        4 << 30, **static,
    )
    (attended_got,) = call(
        got_body,
        [(rows, width)],
        [VMEM],
        [whole(projection, 2 * width), *window, *flash, sems((n + 2,))],
        [
            info, their_lists, their_counts, far_near, q_got, k_near, v_near, gain, *proj
        ],
        [SMEM, SMEM, SMEM, VMEM, VMEM, ANY, ANY, VMEM] + [ANY] * n,
        4 << 30, **static,
    )
    attended_back = send("mesh", swap, attended_got)
    middle_k, hidden_k = call(
        keep_body,
        [(rows, width), (rows, hidden)],
        [VMEM, VMEM],
        [
            whole(projection, 2 * width),
            whole(output_weight, width),
            whole(up_weight, hidden),
            *window,
            pltpu.VMEM((rows, width), BF16),
            *flash,
            sems((3 * n + 2,)),
        ],
        [
            info, tile_lists, tile_counts, keep, far_late, q_keep, k_near, v_near,
            gain, second, *proj, *outs, *ups,
        ],
        [SMEM, SMEM, SMEM, VMEM, VMEM, VMEM, ANY, ANY, VMEM, VMEM] + [ANY] * (3 * n),
        6 << 30, **static,
    )
    middle_g, hidden_g = call(
        back_body,
        [(rows, width), (rows, hidden)],
        [VMEM, VMEM],
        [whole(output_weight, width), whole(up_weight, hidden), sems((2 * n,))],
        [info, give, attended_back, second, *outs, *ups],
        [SMEM, VMEM, VMEM, VMEM] + [ANY] * (2 * n),
        2 << 30, n_pieces=n,
    )
    (result,) = call(
        down_body,
        [node_states.shape],
        [VMEM],
        [
            pltpu.VMEM((n, *down_weight.shape), BF16),
            pltpu.VMEM((2, rows, width), F32),
            sems((n,)),
        ],
        [info, middle_k, hidden_k, middle_g, hidden_g, *downs],
        [SMEM, VMEM, VMEM, VMEM, VMEM] + [ANY] * n,
        2 << 30, n_pieces=n,
    )
    return result


def solution(mesh):
    in_specs = (
        P("member", "mesh", None),
        P("member", None),
        P("member", None),
        P("member", None),
        P("member", None),
        P(),
        P(),
        P("mesh", None),
        P("mesh"),
    )
    return jax.shard_map(
        layer, mesh=mesh, in_specs=in_specs,
        out_specs=P("member", "mesh", None), check_vma=False,
    )
```

```python
import functools
import math

import jax
import jax.numpy as jnp
from jax import lax
from jax.experimental import pallas as pl
from jax.experimental.pallas import tpu as pltpu
from jax.sharding import PartitionSpec as P

HEADS = 4
RIM_T = 4
EXTRA = 16
SURE = 4
BF16 = jnp.bfloat16
F32 = jnp.float32
VMEM = pltpu.VMEM
ANY = pl.ANY
HBM = pltpu.HBM


def norm_rows(rows, gain):
    values = rows.astype(F32)
    center = values - jnp.mean(values, axis=-1, keepdims=True)
    spread = jnp.mean(center * center, axis=-1, keepdims=True)
    return (center * lax.rsqrt(spread + 1e-05) * gain).astype(BF16)


def dot(a, b):
    return lax.dot_general(a, b, (((1,), (0,)), ((), ())), preferred_element_type=F32)


def dot_t(a, b):
    return lax.dot_general(a, b, (((1,), (1,)), ((), ())), preferred_element_type=F32)


def gelu(x):
    linear = math.sqrt(2 / math.pi)
    half = 0.5 * x
    return half + half * jnp.tanh(x * (linear + (0.044715 * linear) * (x * x)))


def places(count, block):
    me = lax.axis_index("member")
    return [pl.multiple_of((me ^ k) * block, block) for k in range(count)]


def stacked(pieces, cols=slice(None)):
    return jnp.concatenate([piece[:, cols] for piece in pieces], axis=0)


def matched(rows, pieces):
    block = pieces[0].shape[0]
    return jnp.concatenate(
        [rows[:, pl.ds(at, block)] for at in places(len(pieces), block)], axis=1
    )


def norm_matched(source, gain, target, pieces):
    block = pieces[0].shape[0]
    me = lax.axis_index("member")
    step = 128
    for r in range(0, target.shape[0], step):
        normed = norm_rows(source[r : r + step, :], gain[...])
        for k in range(len(pieces)):
            target[r : r + step, pl.ds(pl.multiple_of((me ^ k) * block, block), block)] = normed[
                :, k * block : (k + 1) * block
            ]


def project(normed, pieces, queries, keys, values, key_row, first_tile, tile_rows):
    count, width = normed.shape
    rows = normed[...]
    if queries is not None:
        queries[...] = dot(rows, stacked(pieces, slice(0, width))).astype(BF16)
    keys[pl.ds(key_row, count), :] = dot(
        rows, stacked(pieces, slice(width, 2 * width))
    ).astype(BF16)
    block = dot(rows, stacked(pieces, slice(2 * width, 3 * width))).astype(BF16)
    for t in range(count // tile_rows):
        values[first_tile + t] = block[t * tile_rows : (t + 1) * tile_rows].T


def attend_tiles(plan, q_ref, k_ref, v_ref, out_ref, scores, tops, tile_rows, entries):
    rows, width = q_ref.shape
    tiles = rows // tile_rows
    head = width // HEADS
    scale = math.log2(math.e) / math.sqrt(head)
    zero = jnp.zeros((tile_rows, head), BF16)

    def stage(t, p, at):
        row = pl.multiple_of(t * tile_rows, tile_rows)
        first = q_ref[pl.ds(row, tile_rows), 2 * p * head : (2 * p + 1) * head]
        second = q_ref[pl.ds(row, tile_rows), (2 * p + 1) * head : (2 * p + 2) * head]
        both = jnp.concatenate(
            [jnp.concatenate([first, zero], 1), jnp.concatenate([zero, second], 1)], 0
        )
        cols = slice(2 * p * head, (2 * p + 2) * head)
        keys = jnp.concatenate(
            [
                k_ref[pl.ds(pl.multiple_of(plan[t, j] * tile_rows, tile_rows), tile_rows), cols]
                for j in range(entries)
            ],
            0,
        )
        product = dot_t(keys, both)
        scores[at] = product
        top = None
        for j in range(entries):
            part = product[j * tile_rows : (j + 1) * tile_rows]
            part = jnp.max(part.reshape(tile_rows // 8, 8, 2 * tile_rows), axis=0)
            if j >= SURE:
                part = jnp.where(j < plan[8, t], part, -jnp.inf)
            top = part if top is None else jnp.maximum(top, part)
        top = jnp.max(top, axis=0, keepdims=True) * scale
        tops[at] = jnp.broadcast_to(top, tops.shape[1:])

    def blend(t, p, at):
        row = pl.multiple_of(t * tile_rows, tile_rows)
        top = tops[at, 0:1]
        total, outs = None, [None, None]
        for pair in range(0, entries, 2):
            weights = []
            for j in (pair, pair + 1):
                highest = jnp.where(j < plan[8, t], top, jnp.inf) if j >= SURE else top
                weight = jnp.exp2(scores[at, j * tile_rows : (j + 1) * tile_rows] * scale - highest)
                part = jnp.sum(weight.reshape(tile_rows // 8, 8, 2 * tile_rows), axis=0)
                total = part if total is None else total + part
                weights.append(weight.astype(BF16))
            weights = jnp.concatenate(weights, 0)
            for a in range(2):
                h = 2 * p + a
                values = jnp.concatenate(
                    [
                        v_ref[plan[t, j], h * head : (h + 1) * head, :]
                        for j in (pair, pair + 1)
                    ],
                    1,
                )
                out = dot(values, weights[:, a * tile_rows : (a + 1) * tile_rows])
                outs[a] = out if outs[a] is None else outs[a] + out
        total = jnp.sum(total, axis=0, keepdims=True)
        for a in range(2):
            h = 2 * p + a
            out = outs[a] / total[:, a * tile_rows : (a + 1) * tile_rows]
            out_ref[pl.ds(row, tile_rows), h * head : (h + 1) * head] = out.T.astype(BF16)

    pairs = HEADS // 2
    stage(0, 0, 0)

    def one_tile(t, carry):
        for p in range(pairs):
            last = p == pairs - 1
            following = jnp.minimum(t + 1, tiles - 1) if last else t
            stage(following, 0 if last else p + 1, (p + 1) % 2)
            blend(t, p, p % 2)
        return carry

    lax.fori_loop(0, tiles, one_tile, 0)


def slot_rows(lists, counts, place, ring, own_block):
    tiles, _ = lists.shape
    ids = lists[...]
    other = place ^ 1
    third = lax.rem(place + jnp.where(place & 1 == 1, 1, ring - 1), jnp.int32(ring))

    def inside(device):
        inner = ids - device * tiles
        return (inner >= 0) & (inner < tiles), inner

    mine, inner = inside(place)
    theirs, inner_theirs = inside(other)
    slots = jnp.where(
        mine,
        inner + own_block * tiles,
        jnp.where(
            theirs, inner_theirs + (1 - own_block) * tiles, ids - third * tiles + 2 * tiles
        ),
    )
    return jnp.clip(slots, 0, 3 * tiles - 1).astype(F32), counts[...].astype(F32)


def write_table(target, row, slots, counts):
    target[pl.ds(row, EXTRA), :] = jnp.zeros((EXTRA, target.shape[1]), BF16)
    table = jnp.concatenate(
        [
            jnp.pad(slots, ((0, 8 - slots.shape[0]), (0, 128 - slots.shape[1]))),
            jnp.pad(counts, ((0, 7), (0, 128 - counts.shape[1]))),
        ],
        axis=0,
    )
    target[pl.ds(row, EXTRA), 0:128] = table.astype(BF16)


def pack_body(
    states, lists_in, counts_in, gains_in, more_gains_in, give, keep, table, gains, more_gains,
    lists, counts, sems, *, ring,
):
    place = lax.axis_index("mesh")
    side = place & 1
    rows = keep.shape[0]
    copies = [
        pltpu.make_async_copy(lists_in, lists, sems.at[0]),
        pltpu.make_async_copy(counts_in, counts, sems.at[1]),
        pltpu.make_async_copy(states.at[1 - side], give.at[pl.ds(0, rows)], sems.at[2]),
        pltpu.make_async_copy(states.at[side], keep, sems.at[3]),
        pltpu.make_async_copy(gains_in, gains, sems.at[4]),
        pltpu.make_async_copy(more_gains_in, more_gains, sems.at[5]),
    ]
    for copy in copies:
        copy.start()
    for copy in copies[:2]:
        copy.wait()
    write_table(table, 0, *slot_rows(lists, counts, place, ring, 0))
    write_table(give, rows, *slot_rows(lists, counts, place, ring, 1))
    for copy in copies[2:]:
        copy.wait()


def stage_body(source, target, sem):
    copy = pltpu.make_async_copy(source, target, sem)
    copy.start()
    copy.wait()


def near_body(source, gain, *rest, n_pieces, tile_rows):
    pieces, (queries, keys, values, normed) = rest[:n_pieces], rest[n_pieces:]
    norm_matched(source, gain, normed, pieces)
    project(normed, pieces, queries, keys, values, 0, 0, tile_rows)


def reach_body(
    table, far, queries, k_keep, v_keep, k_got, v_got, gain, *rest,
    n_pieces, tile_rows, entries,
):
    pieces, (attended, keys, values, normed, scores, tops, whole, plan, sems) = (
        rest[:n_pieces],
        rest[n_pieces:],
    )
    rows = queries.shape[0]
    tiles = rows // tile_rows
    last = table.shape[0] - EXTRA
    whole[...] = table[last:, 0:128].astype(F32).astype(jnp.int32)
    copies = [
        pltpu.make_async_copy(whole, plan, sems.at[0]),
        pltpu.make_async_copy(k_keep, keys.at[pl.ds(0, rows)], sems.at[1]),
        pltpu.make_async_copy(v_keep, values.at[pl.ds(0, tiles)], sems.at[2]),
        pltpu.make_async_copy(k_got, keys.at[pl.ds(rows, rows)], sems.at[3]),
        pltpu.make_async_copy(v_got, values.at[pl.ds(tiles, tiles)], sems.at[4]),
    ]
    for copy in copies:
        copy.start()
    norm_matched(far, gain, normed, pieces)
    project(normed, pieces, None, keys, values, 2 * rows, 2 * tiles, tile_rows)
    for copy in copies:
        copy.wait()
    attend_tiles(
        plan, queries, keys, values, attended, scores, tops, tile_rows, entries
    )


def widen_body(states, attended, gain, *rest, n_pieces):
    outs, ups = (rest[i * n_pieces : (i + 1) * n_pieces] for i in range(2))
    middle, hidden, mid_scratch, normed = rest[2 * n_pieces :]
    rows = attended.shape[0]
    for r in range(0, rows, 128):
        at = pl.ds(r, 128)
        mid = states[at, :].astype(F32) + dot(matched(attended.at[at], outs), stacked(outs))
        middle[at, :] = mid.astype(BF16)
        mid_scratch[at, :] = mid.astype(BF16)
    norm_matched(mid_scratch, gain, normed, ups)
    for c in range(0, hidden.shape[1], 256):
        cols = slice(c, c + 256)
        hidden[:, cols] = gelu(dot(normed[...], stacked(ups, cols))).astype(BF16)


def down_body(middle_k, hidden_k, middle_g, hidden_g, *rest, n_pieces):
    pieces, (out, staged, sems) = rest[:n_pieces], rest[n_pieces:]
    side = lax.axis_index("mesh") & 1
    starts = places(n_pieces, pieces[0].shape[0])
    rows = middle_k.shape[0]
    step = 256
    copies = []
    for member, middle, hidden in ((side, middle_k, hidden_k), (1 - side, middle_g, hidden_g)):
        for r in range(0, rows, step):
            at = pl.ds(r, step)
            total = middle[at, :].astype(F32)
            for start, piece in zip(starts, pieces):
                total = total + dot(hidden[at, pl.ds(start, piece.shape[0])], piece[...])
            where = len(copies)
            staged[where] = total.astype(BF16)
            copies.append(
                pltpu.make_async_copy(staged.at[where], out.at[member, at], sems.at[where])
            )
            copies[-1].start()
    for copy in copies:
        copy.wait()


def call(body, outs, scratch, operands, spaces, flops, space=VMEM, moved=4 << 20, **static):
    return pl.pallas_call(
        functools.partial(body, **static),
        out_shape=[
            jax.ShapeDtypeStruct(
                [d for d in shape if isinstance(d, int)],
                BF16 if isinstance(shape[-1], int) else shape[-1],
            )
            for shape in outs
        ],
        in_specs=[pl.BlockSpec(memory_space=space) for space in spaces],
        out_specs=[pl.BlockSpec(memory_space=space) for _ in outs],
        scratch_shapes=scratch,
        cost_estimate=pl.CostEstimate(
            flops=flops, bytes_accessed=moved, transcendentals=0
        ),
        compiler_params=pltpu.CompilerParams(vmem_limit_bytes=VMEM_LIMIT),
    )(*operands)


VMEM_LIMIT = 24 << 20


def in_hbm(array):
    return pltpu.with_memory_space_constraint(array, HBM)


def send(axis, perm, array):
    return lax.ppermute(array, axis, perm)


def layer(
    node_states, projection, output_weight, up_weight, down_weight,
    attention_gain, feedforward_gain, tile_lists, tile_counts,
):
    members, rows, width = node_states.shape
    tiles, entries = tile_lists.shape
    tile_rows = rows // tiles
    hidden = up_weight.shape[1]
    ring, n = lax.axis_size("mesh"), lax.axis_size("member")
    if members != 2 or ring % 2 or ring < 4 or n & (n - 1) or RIM_T > tiles or tiles > 8:
        raise ValueError("unsupported mesh")
    bits = [1 << b for b in reversed(range(n.bit_length() - 1))]
    swap = [(i, i ^ 1) for i in range(ring)]
    outward = [(i, (i + (2 if i % 2 else -2)) % ring) for i in range(ring)]
    inward = [(i, (i + (-2 if i % 2 else 2)) % ring) for i in range(ring)]

    def gather(shard):
        pieces = {0: shard}
        for bit in bits:
            perm = [(i, i ^ bit) for i in range(n)]
            for k, piece in list(pieces.items()):
                pieces[k ^ bit] = send("member", perm, piece)
        return [pieces[k] for k in range(n)]

    give, keep, table, gain, second = call(
        pack_body,
        [(rows + EXTRA, width), (rows, width), (EXTRA, width), (1, width, F32), (1, width, F32)],
        [
            pltpu.VMEM((tiles, entries), jnp.int32),
            pltpu.VMEM((1, tiles), jnp.int32),
            pltpu.SemaphoreType.DMA((6,)),
        ],
        [
            in_hbm(x)
            for x in (
                node_states, tile_lists, tile_counts.reshape(1, tiles),
                attention_gain.reshape(1, width), feedforward_gain.reshape(1, width),
            )
        ],
        [HBM] * 5,
        1 << 20, moved=0, ring=ring,
    )
    got = send("mesh", swap, give)
    proj = gather(projection)
    far_near = send("mesh", outward, keep)
    far_late = send("mesh", inward, got)
    outs = gather(output_weight)
    ups = gather(up_weight)
    downs = gather(down_weight)

    block = pltpu.VMEM((rows, width), BF16)
    window = [
        pltpu.VMEM((3 * rows, width), BF16),
        pltpu.VMEM((3 * tiles, width, tile_rows), BF16),
        block,
        pltpu.VMEM((2, entries * tile_rows, 2 * tile_rows), F32),
        pltpu.VMEM((2, 8, 2 * tile_rows), F32),
        pltpu.VMEM((EXTRA, 128), jnp.int32),
        pltpu.SMEM((EXTRA, 128), jnp.int32),
        pltpu.SemaphoreType.DMA((5,)),
    ]

    (own,) = call(
        stage_body,
        [projection.shape],
        [pltpu.SemaphoreType.DMA],
        [in_hbm(projection)],
        [HBM],
        1 << 20, moved=0,
    )
    proj = [own, *proj[1:]]

    def near(source):
        return call(
            near_body,
            [(rows, width), (rows, width), (tiles, width, tile_rows)],
            [block],
            [source, gain, *proj],
            [VMEM] * (2 + n),
            2 << 30, n_pieces=n, tile_rows=tile_rows,
        )

    def reach(table, far, queries):
        (attended,) = call(
            reach_body,
            [(rows, width)],
            window,
            [table, far, queries, k_keep, v_keep, k_got, v_got, gain, *proj],
            [VMEM, VMEM, VMEM, ANY, ANY, ANY, ANY, VMEM] + [VMEM] * n,
            4 << 30, n_pieces=n, tile_rows=tile_rows, entries=entries,
        )
        return attended

    def widen(states, attended):
        return call(
            widen_body,
            [(rows, width), (rows, hidden)],
            [block, block],
            [states, attended, second, *outs, *ups],
            [VMEM] * (3 + 2 * n),
            3 << 30, n_pieces=n,
        )

    q_keep, k_keep, v_keep = near(keep)
    q_got, k_got, v_got = near(got)
    attended_got = reach(got, far_near, q_got)
    attended_back = send("mesh", swap, attended_got)
    attended_keep = reach(table, far_late, q_keep)
    middle_k, hidden_k = widen(keep, attended_keep)
    middle_g, hidden_g = widen(give, attended_back)
    step = math.gcd(rows, 256)
    (result,) = call(
        down_body,
        [node_states.shape],
        [
            pltpu.VMEM((2 * rows // step, step, width), BF16),
            pltpu.SemaphoreType.DMA((2 * rows // step,)),
        ],
        [middle_k, hidden_k, middle_g, hidden_g, *downs],
        [VMEM] * (4 + n),
        4 << 30, space=ANY, n_pieces=n,
    )
    return result


def solution(mesh):
    in_specs = (
        P("member", "mesh", None),
        P("member", None),
        P("member", None),
        P("member", None),
        P("member", None),
        P(),
        P(),
        P("mesh", None),
        P("mesh"),
    )
    return jax.shard_map(
        layer, mesh=mesh, in_specs=in_specs,
        out_specs=P("member", "mesh", None), check_vma=False,
    )
```

```python
import functools
import math

import jax
import jax.numpy as jnp
from jax import lax
from jax.experimental import pallas as pl
from jax.experimental.pallas import tpu as pltpu
from jax.sharding import PartitionSpec as P

HEADS = 4
RIM_T = 4
EXTRA = 16
SURE = 4
BF16 = jnp.bfloat16
F32 = jnp.float32
VMEM = pltpu.VMEM
ANY = pl.ANY
HBM = pltpu.HBM


def norm_rows(rows, gain):
    values = rows.astype(F32)
    center = values - jnp.mean(values, axis=-1, keepdims=True)
    spread = jnp.mean(center * center, axis=-1, keepdims=True)
    return (center * lax.rsqrt(spread + 1e-05) * gain).astype(BF16)


def dot(a, b):
    return lax.dot_general(a, b, (((1,), (0,)), ((), ())), preferred_element_type=F32)


def dot_t(a, b):
    return lax.dot_general(a, b, (((1,), (1,)), ((), ())), preferred_element_type=F32)


def gelu(x):
    linear = math.sqrt(2 / math.pi)
    half = 0.5 * x
    return half + half * jnp.tanh(x * (linear + (0.044715 * linear) * (x * x)))


def places(count, block):
    me = lax.axis_index("member")
    return [pl.multiple_of((me ^ k) * block, block) for k in range(count)]


def stacked(pieces, cols=slice(None)):
    return jnp.concatenate([piece[:, cols] for piece in pieces], axis=0)


def matched(rows, pieces):
    block = pieces[0].shape[0]
    return jnp.concatenate(
        [rows[:, pl.ds(at, block)] for at in places(len(pieces), block)], axis=1
    )


def norm_matched(source, gain, target, pieces):
    block = pieces[0].shape[0]
    me = lax.axis_index("member")
    step = 128
    for r in range(0, target.shape[0], step):
        normed = norm_rows(source[r : r + step, :], gain[...])
        for k in range(len(pieces)):
            target[r : r + step, pl.ds(pl.multiple_of((me ^ k) * block, block), block)] = normed[
                :, k * block : (k + 1) * block
            ]


def project(normed, pieces, queries, keys, values, key_row, first_tile, tile_rows):
    count, width = normed.shape
    rows = normed[...]
    if queries is not None:
        queries[...] = dot(rows, stacked(pieces, slice(0, width))).astype(BF16)
    keys[pl.ds(key_row, count), :] = dot(
        rows, stacked(pieces, slice(width, 2 * width))
    ).astype(BF16)
    block = dot(rows, stacked(pieces, slice(2 * width, 3 * width))).astype(BF16)
    for t in range(count // tile_rows):
        values[first_tile + t] = block[t * tile_rows : (t + 1) * tile_rows].T


def attend_tiles(plan, q_ref, k_ref, v_ref, out_ref, scores, tops, sums, totals, tile_rows, entries):
    rows, width = q_ref.shape
    tiles = rows // tile_rows
    head = width // HEADS
    scale = math.log2(math.e) / math.sqrt(head)
    zero = jnp.zeros((tile_rows, head), BF16)

    def stage(t, p, at):
        row = pl.multiple_of(t * tile_rows, tile_rows)
        first = q_ref[pl.ds(row, tile_rows), 2 * p * head : (2 * p + 1) * head]
        second = q_ref[pl.ds(row, tile_rows), (2 * p + 1) * head : (2 * p + 2) * head]
        both = jnp.concatenate(
            [jnp.concatenate([first, zero], 1), jnp.concatenate([zero, second], 1)], 0
        )
        cols = slice(2 * p * head, (2 * p + 2) * head)
        keys = jnp.concatenate(
            [
                k_ref[pl.ds(pl.multiple_of(plan[t, j] * tile_rows, tile_rows), tile_rows), cols]
                for j in range(entries)
            ],
            0,
        )
        product = dot_t(keys, both)
        scores[at] = product
        top = None
        for j in range(entries):
            part = product[j * tile_rows : (j + 1) * tile_rows]
            part = jnp.max(part.reshape(tile_rows // 8, 8, 2 * tile_rows), axis=0)
            if j >= SURE:
                part = jnp.where(j < plan[8, t], part, -jnp.inf)
            top = part if top is None else jnp.maximum(top, part)
        tops[at] = top

    def blend(t, p, at):
        top = jnp.max(tops[at], axis=0, keepdims=True) * scale
        total, outs = None, [None, None]
        for pair in range(0, entries, 2):
            weights = []
            for j in (pair, pair + 1):
                highest = jnp.where(j < plan[8, t], top, jnp.inf) if j >= SURE else top
                weight = jnp.exp2(scores[at, j * tile_rows : (j + 1) * tile_rows] * scale - highest)
                part = jnp.sum(weight.reshape(tile_rows // 8, 8, 2 * tile_rows), axis=0)
                total = part if total is None else total + part
                weights.append(weight.astype(BF16))
            weights = jnp.concatenate(weights, 0)
            for a in range(2):
                h = 2 * p + a
                values = jnp.concatenate(
                    [v_ref[plan[t, j], h * head : (h + 1) * head, :] for j in (pair, pair + 1)], 1
                )
                out = dot(values, weights[:, a * tile_rows : (a + 1) * tile_rows])
                outs[a] = out if outs[a] is None else outs[a] + out
        totals[at] = total
        for a in range(2):
            sums[at, a * head : (a + 1) * head] = outs[a]

    def finish(t, p, at):
        row = pl.multiple_of(t * tile_rows, tile_rows)
        total = jnp.sum(totals[at], axis=0, keepdims=True)
        for a in range(2):
            h = 2 * p + a
            out = sums[at, a * head : (a + 1) * head] / total[:, a * tile_rows : (a + 1) * tile_rows]
            out_ref[pl.ds(row, tile_rows), h * head : (h + 1) * head] = out.T.astype(BF16)

    pairs = HEADS // 2
    totals[...] = jnp.ones(totals.shape, F32)
    sums[...] = jnp.zeros(sums.shape, F32)
    stage(0, 0, 0)

    def one_tile(t, carry):
        for p in range(pairs):
            last = p == pairs - 1
            following = jnp.minimum(t + 1, tiles - 1) if last else t
            stage(following, 0 if last else p + 1, (p + 1) % 2)
            blend(t, p, p % 2)
            before = jnp.maximum(t - 1, 0) if p == 0 else t
            finish(before, (p - 1) % pairs, (p + 1) % 2)
        return carry

    lax.fori_loop(0, tiles, one_tile, 0, unroll=2 if tiles % 2 == 0 else 1)
    finish(tiles - 1, pairs - 1, (pairs - 1) % 2)


def slot_rows(lists, counts, place, ring, own_block):
    tiles, _ = lists.shape
    ids = lists[...]
    other = place ^ 1
    third = lax.rem(place + jnp.where(place & 1 == 1, 1, ring - 1), jnp.int32(ring))

    def inside(device):
        inner = ids - device * tiles
        return (inner >= 0) & (inner < tiles), inner

    mine, inner = inside(place)
    theirs, inner_theirs = inside(other)
    slots = jnp.where(
        mine,
        inner + own_block * tiles,
        jnp.where(
            theirs, inner_theirs + (1 - own_block) * tiles, ids - third * tiles + 2 * tiles
        ),
    )
    return jnp.clip(slots, 0, 3 * tiles - 1).astype(F32), counts[...].astype(F32)


def write_table(target, row, slots, counts):
    target[pl.ds(row, EXTRA), :] = jnp.zeros((EXTRA, target.shape[1]), BF16)
    table = jnp.concatenate(
        [
            jnp.pad(slots, ((0, 8 - slots.shape[0]), (0, 128 - slots.shape[1]))),
            jnp.pad(counts, ((0, 7), (0, 128 - counts.shape[1]))),
        ],
        axis=0,
    )
    target[pl.ds(row, EXTRA), 0:128] = table.astype(BF16)


def pack_body(
    states, lists_in, counts_in, gains_in, more_gains_in, give, keep, table, gains, more_gains,
    lists, counts, sems, *, ring,
):
    place = lax.axis_index("mesh")
    side = place & 1
    rows = keep.shape[0]
    copies = [
        pltpu.make_async_copy(lists_in, lists, sems.at[0]),
        pltpu.make_async_copy(counts_in, counts, sems.at[1]),
        pltpu.make_async_copy(states.at[1 - side], give.at[pl.ds(0, rows)], sems.at[2]),
        pltpu.make_async_copy(states.at[side], keep, sems.at[3]),
        pltpu.make_async_copy(gains_in, gains, sems.at[4]),
        pltpu.make_async_copy(more_gains_in, more_gains, sems.at[5]),
    ]
    for copy in copies:
        copy.start()
    for copy in copies[:2]:
        copy.wait()
    write_table(table, 0, *slot_rows(lists, counts, place, ring, 0))
    write_table(give, rows, *slot_rows(lists, counts, place, ring, 1))
    for copy in copies[2:]:
        copy.wait()


def stage_body(source, target, sem):
    copy = pltpu.make_async_copy(source, target, sem)
    copy.start()
    copy.wait()


def near_body(source, gain, *rest, n_pieces, tile_rows):
    pieces, (queries, keys, values, normed) = rest[:n_pieces], rest[n_pieces:]
    norm_matched(source, gain, normed, pieces)
    project(normed, pieces, queries, keys, values, 0, 0, tile_rows)


def reach_body(
    table, far, queries, k_keep, v_keep, k_got, v_got, gain, *rest,
    n_pieces, tile_rows, entries,
):
    pieces, (attended, keys, values, normed, scores, tops, sums, totals, whole, plan, sems) = (
        rest[:n_pieces],
        rest[n_pieces:],
    )
    rows = queries.shape[0]
    tiles = rows // tile_rows
    last = table.shape[0] - EXTRA
    whole[...] = table[last:, 0:128].astype(F32).astype(jnp.int32)
    copies = [
        pltpu.make_async_copy(whole, plan, sems.at[0]),
        pltpu.make_async_copy(k_keep, keys.at[pl.ds(0, rows)], sems.at[1]),
        pltpu.make_async_copy(v_keep, values.at[pl.ds(0, tiles)], sems.at[2]),
        pltpu.make_async_copy(k_got, keys.at[pl.ds(rows, rows)], sems.at[3]),
        pltpu.make_async_copy(v_got, values.at[pl.ds(tiles, tiles)], sems.at[4]),
    ]
    for copy in copies:
        copy.start()
    norm_matched(far, gain, normed, pieces)
    project(normed, pieces, None, keys, values, 2 * rows, 2 * tiles, tile_rows)
    for copy in copies:
        copy.wait()
    attend_tiles(
        plan, queries, keys, values, attended, scores, tops, sums, totals, tile_rows, entries
    )


def middle_rows(states, attended, outs, middle):
    for r in range(0, attended.shape[0], 128):
        at = pl.ds(r, 128)
        mid = states[at, :].astype(F32) + dot(matched(attended.at[at], outs), stacked(outs))
        middle[at, :] = mid.astype(BF16)


def widen_body(states, attended, gain, *rest, n_pieces):
    outs, ups = (rest[i * n_pieces : (i + 1) * n_pieces] for i in range(2))
    middle, hidden, normed = rest[2 * n_pieces :]
    middle_rows(states, attended, outs, middle)
    norm_matched(middle, gain, normed, ups)
    for c in range(0, hidden.shape[1], 256):
        cols = slice(c, c + 256)
        hidden[:, cols] = gelu(dot(normed[...], stacked(ups, cols))).astype(BF16)


def rest_body(states, attended, gain, middle_k, hidden_k, *rest, n_pieces, n_downs):
    outs, ups = (rest[i * n_pieces : (i + 1) * n_pieces] for i in range(2))
    downs = rest[2 * n_pieces : 2 * n_pieces + n_downs]
    middle, hidden, total, normed = rest[2 * n_pieces + n_downs :]
    starts = places(n_downs, downs[0].shape[0])
    middle_rows(states, attended, outs, middle)
    norm_matched(middle, gain, normed, ups)
    chunks = hidden.shape[1] // 256
    units = [(k, h) for k in range(n_downs) for h in range(total.shape[0])]
    per = -(-len(units) // chunks)
    for c in range(chunks):
        wide = slice(c * 256, (c + 1) * 256)
        for k, h in units[c * per : (c + 1) * per]:
            cols = slice(h * 256, (h + 1) * 256)
            part = dot(hidden_k[:, pl.ds(starts[k], downs[k].shape[0])], downs[k][:, cols])
            total[h] = part + (middle_k[:, cols].astype(F32) if k == 0 else total[h])
        hidden[:, wide] = gelu(dot(normed[...], stacked(ups, wide))).astype(BF16)


def last_body(total, hidden_k, middle, hidden, *rest, n_pieces):
    downs, (out, staged, sems) = rest[:n_pieces], rest[n_pieces:]
    side = lax.axis_index("mesh") & 1
    rows = middle.shape[0]
    starts = places(n_pieces, downs[0].shape[0])
    some = hidden_k[:, pl.ds(starts[-1], downs[-1].shape[0])]
    for h in range(total.shape[0]):
        cols = slice(h * 256, (h + 1) * 256)
        staged[0, :, cols] = (total[h] + dot(some, downs[-1][:, cols])).astype(BF16)
    copies = [pltpu.make_async_copy(staged.at[0], out.at[side], sems.at[0])]
    copies[0].start()
    step = 256
    for r in range(0, rows, step):
        at = pl.ds(r, step)
        final = middle[at, :].astype(F32)
        for start, piece in zip(starts, downs):
            final = final + dot(hidden[at, pl.ds(start, piece.shape[0])], piece[...])
        staged[1, at] = final.astype(BF16)
        copies.append(
            pltpu.make_async_copy(staged.at[1, at], out.at[1 - side, at], sems.at[len(copies)])
        )
        copies[-1].start()
    for copy in copies:
        copy.wait()


def call(body, outs, scratch, operands, spaces, flops, space=VMEM, moved=4 << 20, **static):
    return pl.pallas_call(
        functools.partial(body, **static),
        out_shape=[
            jax.ShapeDtypeStruct(
                [d for d in shape if isinstance(d, int)],
                BF16 if isinstance(shape[-1], int) else shape[-1],
            )
            for shape in outs
        ],
        in_specs=[pl.BlockSpec(memory_space=space) for space in spaces],
        out_specs=[pl.BlockSpec(memory_space=space) for _ in outs],
        scratch_shapes=scratch,
        cost_estimate=pl.CostEstimate(
            flops=flops, bytes_accessed=moved, transcendentals=0
        ),
        compiler_params=pltpu.CompilerParams(vmem_limit_bytes=VMEM_LIMIT),
    )(*operands)


VMEM_LIMIT = 24 << 20


def in_hbm(array):
    return pltpu.with_memory_space_constraint(array, HBM)


def send(axis, perm, array):
    return lax.ppermute(array, axis, perm)


def layer(
    node_states, projection, output_weight, up_weight, down_weight,
    attention_gain, feedforward_gain, tile_lists, tile_counts,
):
    members, rows, width = node_states.shape
    tiles, entries = tile_lists.shape
    tile_rows = rows // tiles
    hidden = up_weight.shape[1]
    ring, n = lax.axis_size("mesh"), lax.axis_size("member")
    if members != 2 or ring % 2 or ring < 4 or n & (n - 1) or RIM_T > tiles or tiles > 8:
        raise ValueError("unsupported mesh")
    bits = [1 << b for b in reversed(range(n.bit_length() - 1))]
    swap = [(i, i ^ 1) for i in range(ring)]
    outward = [(i, (i + (2 if i % 2 else -2)) % ring) for i in range(ring)]
    inward = [(i, (i + (-2 if i % 2 else 2)) % ring) for i in range(ring)]

    def gather(shard):
        pieces = {0: shard}
        for bit in bits:
            perm = [(i, i ^ bit) for i in range(n)]
            for k, piece in list(pieces.items()):
                pieces[k ^ bit] = send("member", perm, piece)
        return [pieces[k] for k in range(n)]

    give, keep, table, gain, second = call(
        pack_body,
        [(rows + EXTRA, width), (rows, width), (EXTRA, width), (1, width, F32), (1, width, F32)],
        [
            pltpu.VMEM((tiles, entries), jnp.int32),
            pltpu.VMEM((1, tiles), jnp.int32),
            pltpu.SemaphoreType.DMA((6,)),
        ],
        [
            in_hbm(x)
            for x in (
                node_states, tile_lists, tile_counts.reshape(1, tiles),
                attention_gain.reshape(1, width), feedforward_gain.reshape(1, width),
            )
        ],
        [HBM] * 5,
        1 << 20, moved=0, ring=ring,
    )
    got = send("mesh", swap, give)
    proj = gather(projection)
    far_near = send("mesh", outward, keep)
    far_late = send("mesh", inward, got)
    outs = gather(output_weight)
    ups = gather(up_weight)
    downs = gather(down_weight)

    block = pltpu.VMEM((rows, width), BF16)
    window = [
        pltpu.VMEM((3 * rows, width), BF16),
        pltpu.VMEM((3 * tiles, width, tile_rows), BF16),
        block,
        pltpu.VMEM((2, entries * tile_rows, 2 * tile_rows), F32),
        pltpu.VMEM((2, 8, 2 * tile_rows), F32),
        pltpu.VMEM((2, 2 * width // HEADS, tile_rows), F32),
        pltpu.VMEM((2, 8, 2 * tile_rows), F32),
        pltpu.VMEM((EXTRA, 128), jnp.int32),
        pltpu.SMEM((EXTRA, 128), jnp.int32),
        pltpu.SemaphoreType.DMA((5,)),
    ]

    (own,) = call(
        stage_body,
        [projection.shape],
        [pltpu.SemaphoreType.DMA],
        [in_hbm(projection)],
        [HBM],
        1 << 20, moved=0,
    )
    proj = [own, *proj[1:]]

    def near(source):
        return call(
            near_body,
            [(rows, width), (rows, width), (tiles, width, tile_rows)],
            [block],
            [source, gain, *proj],
            [VMEM] * (2 + n),
            2 << 30, n_pieces=n, tile_rows=tile_rows,
        )

    def reach(table, far, queries):
        (attended,) = call(
            reach_body,
            [(rows, width)],
            window,
            [table, far, queries, k_keep, v_keep, k_got, v_got, gain, *proj],
            [VMEM, VMEM, VMEM, ANY, ANY, ANY, ANY, VMEM] + [VMEM] * n,
            4 << 30, n_pieces=n, tile_rows=tile_rows, entries=entries,
        )
        return attended

    q_keep, k_keep, v_keep = near(keep)
    q_got, k_got, v_got = near(got)
    attended_got = reach(got, far_near, q_got)
    attended_back = send("mesh", swap, attended_got)
    attended_keep = reach(table, far_late, q_keep)
    middle_k, hidden_k = call(
        widen_body,
        [(rows, width), (rows, hidden)],
        [block],
        [keep, attended_keep, second, *outs, *ups],
        [VMEM] * (3 + 2 * n),
        3 << 30, n_pieces=n,
    )
    middle_g, hidden_g, total = call(
        rest_body,
        [(rows, width), (rows, hidden), (width // 256, rows, 256, F32)],
        [block],
        [give, attended_back, second, middle_k, hidden_k, *outs, *ups, *downs[:-1]],
        [VMEM] * (4 + 3 * n),
        5 << 30, n_pieces=n, n_downs=n - 1,
    )
    (result,) = call(
        last_body,
        [node_states.shape],
        [pltpu.VMEM((2, rows, width), BF16), pltpu.SemaphoreType.DMA((1 + rows // 256,))],
        [total, hidden_k, middle_g, hidden_g, *downs],
        [VMEM] * (4 + n),
        3 << 30, space=ANY, n_pieces=n,
    )
    return result


def solution(mesh):
    in_specs = (
        P("member", "mesh", None),
        P("member", None),
        P("member", None),
        P("member", None),
        P("member", None),
        P(),
        P(),
        P("mesh", None),
        P("mesh"),
    )
    return jax.shard_map(
        layer, mesh=mesh, in_specs=in_specs,
        out_specs=P("member", "mesh", None), check_vma=False,
    )
```

```python
import functools
import math

import jax
import jax.numpy as jnp
from jax import lax
from jax.experimental import pallas as pl
from jax.experimental.pallas import tpu as pltpu
from jax.sharding import PartitionSpec as P

HEADS = 4
RIM_T = 4
EXTRA = 16
SURE = 4
BF16 = jnp.bfloat16
F32 = jnp.float32
VMEM = pltpu.VMEM
ANY = pl.ANY
HBM = pltpu.HBM


def norm_rows(rows, gain):
    values = rows.astype(F32)
    center = values - jnp.mean(values, axis=-1, keepdims=True)
    spread = jnp.mean(center * center, axis=-1, keepdims=True)
    return (center * lax.rsqrt(spread + 1e-05) * gain).astype(BF16)


def dot(a, b):
    return lax.dot_general(a, b, (((1,), (0,)), ((), ())), preferred_element_type=F32)


def dot_t(a, b):
    return lax.dot_general(a, b, (((1,), (1,)), ((), ())), preferred_element_type=F32)


def gelu(x):
    linear = math.sqrt(2 / math.pi)
    half = 0.5 * x
    return half + half * jnp.tanh(x * (linear + (0.044715 * linear) * (x * x)))


def places(count, block):
    me = lax.axis_index("member")
    return [pl.multiple_of((me ^ k) * block, block) for k in range(count)]


def stacked(pieces, cols=slice(None)):
    return jnp.concatenate([piece[:, cols] for piece in pieces], axis=0)


def matched(rows, pieces):
    block = pieces[0].shape[0]
    return jnp.concatenate(
        [rows[:, pl.ds(at, block)] for at in places(len(pieces), block)], axis=1
    )


def norm_matched(source, gain, target, pieces, span=None):
    block = pieces[0].shape[0]
    me = lax.axis_index("member")
    step = 128
    for r in range(*(span or (0, target.shape[0])), step):
        normed = norm_rows(source[r : r + step, :], gain[...])
        for k in range(len(pieces)):
            target[r : r + step, pl.ds(pl.multiple_of((me ^ k) * block, block), block)] = normed[
                :, k * block : (k + 1) * block
            ]


def norm_project(source, gain, normed, pieces, queries, keys, values, third, tile_rows):
    count, width = normed.shape
    step = count // 2
    for r in range(0, count, step):
        norm_matched(source, gain, normed, pieces, (r, r + step))
        at = pl.ds(r, step)
        rows = normed[at, :]
        if queries is not None:
            queries[at, :] = dot(rows, stacked(pieces, slice(0, width))).astype(BF16)
        keys[pl.ds(third * count + r, step), :] = dot(
            rows, stacked(pieces, slice(width, 2 * width))
        ).astype(BF16)
        block = dot(rows, stacked(pieces, slice(2 * width, 3 * width))).astype(BF16)
        for t in range(step // tile_rows):
            slot = (third * count + r) // tile_rows + t
            values[slot] = block[t * tile_rows : (t + 1) * tile_rows].T


def attend_tiles(plan, q_ref, k_ref, v_ref, out_ref, scores, tops, sums, totals, tile_rows, entries):
    rows, width = q_ref.shape
    tiles = rows // tile_rows
    head = width // HEADS
    scale = math.log2(math.e) / math.sqrt(head)
    zero = jnp.zeros((tile_rows, head), BF16)

    def stage(t, p, at):
        row = pl.multiple_of(t * tile_rows, tile_rows)
        first = q_ref[pl.ds(row, tile_rows), 2 * p * head : (2 * p + 1) * head]
        second = q_ref[pl.ds(row, tile_rows), (2 * p + 1) * head : (2 * p + 2) * head]
        both = jnp.concatenate(
            [jnp.concatenate([first, zero], 1), jnp.concatenate([zero, second], 1)], 0
        )
        cols = slice(2 * p * head, (2 * p + 2) * head)
        keys = jnp.concatenate(
            [
                k_ref[pl.ds(pl.multiple_of(plan[t, j] * tile_rows, tile_rows), tile_rows), cols]
                for j in range(entries)
            ],
            0,
        )
        product = dot_t(keys, both)
        scores[at] = product
        top = None
        for j in range(entries):
            part = product[j * tile_rows : (j + 1) * tile_rows]
            part = jnp.max(part.reshape(tile_rows // 8, 8, 2 * tile_rows), axis=0)
            if j >= SURE:
                part = jnp.where(j < plan[8, t], part, -jnp.inf)
            top = part if top is None else jnp.maximum(top, part)
        tops[at] = top

    def blend(t, p, at):
        top = jnp.max(tops[at], axis=0, keepdims=True) * scale
        total, outs = None, [None, None]
        for pair in range(0, entries, 2):
            weights = []
            for j in (pair, pair + 1):
                highest = jnp.where(j < plan[8, t], top, jnp.inf) if j >= SURE else top
                weight = jnp.exp2(scores[at, j * tile_rows : (j + 1) * tile_rows] * scale - highest)
                part = jnp.sum(weight.reshape(tile_rows // 8, 8, 2 * tile_rows), axis=0)
                total = part if total is None else total + part
                weights.append(weight.astype(BF16))
            weights = jnp.concatenate(weights, 0)
            for a in range(2):
                h = 2 * p + a
                values = jnp.concatenate(
                    [v_ref[plan[t, j], h * head : (h + 1) * head, :] for j in (pair, pair + 1)], 1
                )
                out = dot(values, weights[:, a * tile_rows : (a + 1) * tile_rows])
                outs[a] = out if outs[a] is None else outs[a] + out
        totals[at] = total
        for a in range(2):
            sums[at, a * head : (a + 1) * head] = outs[a]

    def finish(t, p, at):
        row = pl.multiple_of(t * tile_rows, tile_rows)
        total = jnp.sum(totals[at], axis=0, keepdims=True)
        for a in range(2):
            h = 2 * p + a
            out = sums[at, a * head : (a + 1) * head] / total[:, a * tile_rows : (a + 1) * tile_rows]
            out_ref[pl.ds(row, tile_rows), h * head : (h + 1) * head] = out.T.astype(BF16)

    pairs = HEADS // 2
    totals[...] = jnp.ones(totals.shape, F32)
    sums[...] = jnp.zeros(sums.shape, F32)
    stage(0, 0, 0)

    def one_tile(t, carry):
        for p in range(pairs):
            last = p == pairs - 1
            following = jnp.minimum(t + 1, tiles - 1) if last else t
            stage(following, 0 if last else p + 1, (p + 1) % 2)
            blend(t, p, p % 2)
            before = jnp.maximum(t - 1, 0) if p == 0 else t
            finish(before, (p - 1) % pairs, (p + 1) % 2)
        return carry

    lax.fori_loop(0, tiles, one_tile, 0, unroll=2 if tiles % 2 == 0 else 1)
    finish(tiles - 1, pairs - 1, (pairs - 1) % 2)


def slot_rows(lists, counts, place, ring, own_block):
    tiles, _ = lists.shape
    ids = lists[...]
    other = place ^ 1
    third = lax.rem(place + jnp.where(place & 1 == 1, 1, ring - 1), jnp.int32(ring))

    def inside(device):
        inner = ids - device * tiles
        return (inner >= 0) & (inner < tiles), inner

    mine, inner = inside(place)
    theirs, inner_theirs = inside(other)
    slots = jnp.where(
        mine,
        inner + own_block * tiles,
        jnp.where(
            theirs, inner_theirs + (1 - own_block) * tiles, ids - third * tiles + 2 * tiles
        ),
    )
    return jnp.clip(slots, 0, 3 * tiles - 1).astype(F32), counts[...].astype(F32)


def write_table(target, row, slots, counts):
    target[pl.ds(row, EXTRA), :] = jnp.zeros((EXTRA, target.shape[1]), BF16)
    table = jnp.concatenate(
        [
            jnp.pad(slots, ((0, 8 - slots.shape[0]), (0, 128 - slots.shape[1]))),
            jnp.pad(counts, ((0, 7), (0, 128 - counts.shape[1]))),
        ],
        axis=0,
    )
    target[pl.ds(row, EXTRA), 0:128] = table.astype(BF16)


def pack_body(
    states, lists_in, counts_in, gains_in, more_gains_in, give, keep, table, gains, more_gains,
    lists, counts, sems, *, ring,
):
    place = lax.axis_index("mesh")
    side = place & 1
    rows = keep.shape[0]
    copies = [
        pltpu.make_async_copy(lists_in, lists, sems.at[0]),
        pltpu.make_async_copy(counts_in, counts, sems.at[1]),
        pltpu.make_async_copy(states.at[1 - side], give.at[pl.ds(0, rows)], sems.at[2]),
        pltpu.make_async_copy(states.at[side], keep, sems.at[3]),
        pltpu.make_async_copy(gains_in, gains, sems.at[4]),
        pltpu.make_async_copy(more_gains_in, more_gains, sems.at[5]),
    ]
    for copy in copies:
        copy.start()
    for copy in copies[:2]:
        copy.wait()
    write_table(table, 0, *slot_rows(lists, counts, place, ring, 0))
    write_table(give, rows, *slot_rows(lists, counts, place, ring, 1))
    for copy in copies[2:]:
        copy.wait()


def stage_body(source, target, sem):
    copy = pltpu.make_async_copy(source, target, sem)
    copy.start()
    copy.wait()


def near_body(source, gain, *rest, n_pieces, tile_rows):
    pieces, (queries, keys, values, normed) = rest[:n_pieces], rest[n_pieces:]
    norm_project(source, gain, normed, pieces, queries, keys, values, 0, tile_rows)


def reach_body(
    table, far, queries, k_keep, v_keep, k_got, v_got, gain, *rest,
    n_pieces, tile_rows, entries,
):
    pieces, (attended, keys, values, normed, scores, tops, sums, totals, whole, plan, sems) = (
        rest[:n_pieces],
        rest[n_pieces:],
    )
    rows = queries.shape[0]
    tiles = rows // tile_rows
    last = table.shape[0] - EXTRA
    whole[...] = table[last:, 0:128].astype(F32).astype(jnp.int32)
    copies = [
        pltpu.make_async_copy(whole, plan, sems.at[0]),
        pltpu.make_async_copy(k_keep, keys.at[pl.ds(0, rows)], sems.at[1]),
        pltpu.make_async_copy(v_keep, values.at[pl.ds(0, tiles)], sems.at[2]),
        pltpu.make_async_copy(k_got, keys.at[pl.ds(rows, rows)], sems.at[3]),
        pltpu.make_async_copy(v_got, values.at[pl.ds(tiles, tiles)], sems.at[4]),
    ]
    for copy in copies:
        copy.start()
    norm_project(far, gain, normed, pieces, None, keys, values, 2, tile_rows)
    for copy in copies:
        copy.wait()
    attend_tiles(
        plan, queries, keys, values, attended, scores, tops, sums, totals, tile_rows, entries
    )


def middle_rows(states, attended, outs, middle, span=None):
    for r in range(*(span or (0, attended.shape[0])), 128):
        at = pl.ds(r, 128)
        mid = states[at, :].astype(F32) + dot(matched(attended.at[at], outs), stacked(outs))
        middle[at, :] = mid.astype(BF16)


def widen_chunks(normed, middle, ups, downs, hidden, total, early, aside=()):
    block = downs[0].shape[0]
    step = 256
    starts = places(hidden.shape[1] // block, block)
    aside = list(aside)
    behind = None

    def follow():
        if behind is not None:
            k, i, values = behind
            for h in range(total.shape[0]):
                cols = slice(h * 256, (h + 1) * 256)
                part = dot(values, downs[k][i : i + step, cols])
                base = middle[:, cols].astype(F32) if k == i == 0 else total[h]
                total[h] = base + part

    for k, start in enumerate(starts):
        for i in range(0, block, step):
            cols = pl.ds(pl.multiple_of(start + i, step), step)
            wide = dot(normed[...], stacked(ups, cols))
            follow()
            behind = None
            if aside and k >= early:
                aside.pop(0)()
            values = gelu(wide).astype(BF16)
            hidden[:, cols] = values
            if k < early:
                behind = (k, i, values)
    follow()
    for unit in aside:
        unit()


def widen_body(states, attended, gain, *rest, n_pieces, early):
    outs, ups = (rest[i * n_pieces : (i + 1) * n_pieces] for i in range(2))
    downs = rest[2 * n_pieces : 2 * n_pieces + early]
    hidden, total, middle, normed = rest[2 * n_pieces + early :]
    middle_rows(states, attended, outs, middle)
    norm_matched(middle, gain, normed, ups)
    widen_chunks(normed, middle, ups, downs, hidden, total, early)


def rest_body(states, attended, gain, hidden_k, total_in, *rest, n_pieces, early):
    outs, ups = (rest[i * n_pieces : (i + 1) * n_pieces] for i in range(2))
    downs = rest[2 * n_pieces : 3 * n_pieces - 1]
    hidden, total_k, total_g, middle, normed = rest[3 * n_pieces - 1 :]
    block = downs[0].shape[0]
    starts = places(n_pieces, block)

    def unit(k, h):
        def run():
            part = dot(hidden_k[:, pl.ds(starts[k], block)], downs[k][:, h * 256 : (h + 1) * 256])
            total_k[h] = part + (total_in[h] if k == early else total_k[h])

        return run

    units = [unit(k, h) for k in range(early, n_pieces - 1) for h in range(total_k.shape[0])]
    for r in range(0, middle.shape[0], 128):
        middle_rows(states, attended, outs, middle, (r, r + 128))
        if r % 256 == 0 and units:
            units.pop(0)()
        norm_matched(middle, gain, normed, ups, (r, r + 128))
    widen_chunks(normed, middle, ups, downs, hidden, total_g, early, units)


def last_body(total_k, total_g, hidden_k, hidden_g, *rest, n_pieces, early):
    late = n_pieces - early
    downs, (out, staged, sems) = rest[:late], rest[late:]
    side = lax.axis_index("mesh") & 1
    rows, _ = staged.shape[1:]
    block = downs[0].shape[0]
    starts = places(n_pieces, block)[early:]
    copies = []
    step = 256
    for i, (total, hidden, member, first) in enumerate(
        ((total_k, hidden_k, side, late - 1), (total_g, hidden_g, 1 - side, 0))
    ):
        for r in range(0, rows, step):
            at = pl.ds(r, step)
            final = None
            for start, piece in list(zip(starts, downs))[first:]:
                part = dot(hidden[at, pl.ds(start, block)], piece[...])
                final = part if final is None else final + part
            for h in range(total.shape[0]):
                cols = slice(h * 256, (h + 1) * 256)
                staged[i, at, cols] = (total[h, at] + final[:, cols]).astype(BF16)
            copies.append(
                pltpu.make_async_copy(staged.at[i, at], out.at[member, at], sems.at[len(copies)])
            )
            copies[-1].start()
    for copy in copies:
        copy.wait()


def call(body, outs, scratch, operands, spaces, flops, space=VMEM, moved=4 << 20, **static):
    return pl.pallas_call(
        functools.partial(body, **static),
        out_shape=[
            jax.ShapeDtypeStruct(
                [d for d in shape if isinstance(d, int)],
                BF16 if isinstance(shape[-1], int) else shape[-1],
            )
            for shape in outs
        ],
        in_specs=[pl.BlockSpec(memory_space=space) for space in spaces],
        out_specs=[pl.BlockSpec(memory_space=space) for _ in outs],
        scratch_shapes=scratch,
        cost_estimate=pl.CostEstimate(
            flops=flops, bytes_accessed=moved, transcendentals=0
        ),
        compiler_params=pltpu.CompilerParams(vmem_limit_bytes=VMEM_LIMIT),
    )(*operands)


VMEM_LIMIT = 24 << 20


def in_hbm(array):
    return pltpu.with_memory_space_constraint(array, HBM)


def send(axis, perm, array):
    return lax.ppermute(array, axis, perm)


def layer(
    node_states, projection, output_weight, up_weight, down_weight,
    attention_gain, feedforward_gain, tile_lists, tile_counts,
):
    members, rows, width = node_states.shape
    tiles, entries = tile_lists.shape
    tile_rows = rows // tiles
    hidden = up_weight.shape[1]
    ring, n = lax.axis_size("mesh"), lax.axis_size("member")
    if members != 2 or ring % 2 or ring < 4 or n & (n - 1) or RIM_T > tiles or tiles > 8:
        raise ValueError("unsupported mesh")
    bits = [1 << b for b in reversed(range(n.bit_length() - 1))]
    swap = [(i, i ^ 1) for i in range(ring)]
    outward = [(i, (i + (2 if i % 2 else -2)) % ring) for i in range(ring)]
    inward = [(i, (i + (-2 if i % 2 else 2)) % ring) for i in range(ring)]

    def gather(shard):
        pieces = {0: shard}
        for bit in bits:
            perm = [(i, i ^ bit) for i in range(n)]
            for k, piece in list(pieces.items()):
                pieces[k ^ bit] = send("member", perm, piece)
        return [pieces[k] for k in range(n)]

    give, keep, table, gain, second = call(
        pack_body,
        [(rows + EXTRA, width), (rows, width), (EXTRA, width), (1, width, F32), (1, width, F32)],
        [
            pltpu.VMEM((tiles, entries), jnp.int32),
            pltpu.VMEM((1, tiles), jnp.int32),
            pltpu.SemaphoreType.DMA((6,)),
        ],
        [
            in_hbm(x)
            for x in (
                node_states, tile_lists, tile_counts.reshape(1, tiles),
                attention_gain.reshape(1, width), feedforward_gain.reshape(1, width),
            )
        ],
        [HBM] * 5,
        1 << 20, moved=0, ring=ring,
    )
    got = send("mesh", swap, give)
    proj = gather(projection)
    far_near = send("mesh", outward, keep)
    far_late = send("mesh", inward, got)
    outs = gather(output_weight)
    ups = gather(up_weight)
    downs = gather(down_weight)

    block = pltpu.VMEM((rows, width), BF16)
    window = [
        pltpu.VMEM((3 * rows, width), BF16),
        pltpu.VMEM((3 * tiles, width, tile_rows), BF16),
        block,
        pltpu.VMEM((2, entries * tile_rows, 2 * tile_rows), F32),
        pltpu.VMEM((2, 8, 2 * tile_rows), F32),
        pltpu.VMEM((2, 2 * width // HEADS, tile_rows), F32),
        pltpu.VMEM((2, 8, 2 * tile_rows), F32),
        pltpu.VMEM((EXTRA, 128), jnp.int32),
        pltpu.SMEM((EXTRA, 128), jnp.int32),
        pltpu.SemaphoreType.DMA((5,)),
    ]

    (own,) = call(
        stage_body,
        [projection.shape],
        [pltpu.SemaphoreType.DMA],
        [in_hbm(projection)],
        [HBM],
        1 << 20, moved=0,
    )
    proj = [own, *proj[1:]]

    def near(source):
        return call(
            near_body,
            [(rows, width), (rows, width), (tiles, width, tile_rows)],
            [block],
            [source, gain, *proj],
            [VMEM] * (2 + n),
            2 << 30, n_pieces=n, tile_rows=tile_rows,
        )

    def reach(table, far, queries):
        (attended,) = call(
            reach_body,
            [(rows, width)],
            window,
            [table, far, queries, k_keep, v_keep, k_got, v_got, gain, *proj],
            [VMEM, VMEM, VMEM, ANY, ANY, ANY, ANY, VMEM] + [VMEM] * n,
            4 << 30, n_pieces=n, tile_rows=tile_rows, entries=entries,
        )
        return attended

    q_keep, k_keep, v_keep = near(keep)
    q_got, k_got, v_got = near(got)
    attended_got = reach(got, far_near, q_got)
    attended_back = send("mesh", swap, attended_got)
    attended_keep = reach(table, far_late, q_keep)
    early = n // 2
    sums = (width // 256, rows, 256, F32)
    hidden_k, total_k = call(
        widen_body,
        [(rows, hidden), sums],
        [block, block],
        [keep, attended_keep, second, *outs, *ups, *downs[:early]],
        [VMEM] * (3 + 2 * n + early),
        3 << 30, n_pieces=n, early=early,
    )
    hidden_g, total_k, total_g = call(
        rest_body,
        [(rows, hidden), sums, sums],
        [block, block],
        [give, attended_back, second, hidden_k, total_k, *outs, *ups, *downs[:-1]],
        [VMEM] * (4 + 3 * n),
        5 << 30, n_pieces=n, early=early,
    )
    (result,) = call(
        last_body,
        [node_states.shape],
        [pltpu.VMEM((2, rows, width), BF16), pltpu.SemaphoreType.DMA((2 * rows // 256,))],
        [total_k, total_g, hidden_k, hidden_g, *downs[early:]],
        [VMEM] * (4 + n - early),
        2 << 30, space=ANY, n_pieces=n, early=early,
    )
    return result


def solution(mesh):
    in_specs = (
        P("member", "mesh", None),
        P("member", None),
        P("member", None),
        P("member", None),
        P("member", None),
        P(),
        P(),
        P("mesh", None),
        P("mesh"),
    )
    return jax.shard_map(
        layer, mesh=mesh, in_specs=in_specs,
        out_specs=P("member", "mesh", None), check_vma=False,
    )
```

```python
import functools
import math

import jax
import jax.numpy as jnp
from jax import lax
from jax.experimental import pallas as pl
from jax.experimental.pallas import tpu as pltpu
from jax.sharding import PartitionSpec as P

HEADS = 4
RIM_T = 4
EXTRA = 16
SURE = 4
BF16 = jnp.bfloat16
F32 = jnp.float32
VMEM = pltpu.VMEM
ANY = pl.ANY
HBM = pltpu.HBM


def norm_rows(rows, gain):
    values = rows.astype(F32)
    center = values - jnp.mean(values, axis=-1, keepdims=True)
    spread = jnp.mean(center * center, axis=-1, keepdims=True)
    return (center * lax.rsqrt(spread + 1e-05) * gain).astype(BF16)


def dot(a, b):
    return lax.dot_general(a, b, (((1,), (0,)), ((), ())), preferred_element_type=F32)


def dot_t(a, b):
    return lax.dot_general(a, b, (((1,), (1,)), ((), ())), preferred_element_type=F32)


def gelu(x):
    linear = math.sqrt(2 / math.pi)
    half = 0.5 * x
    return half + half * jnp.tanh(x * (linear + (0.044715 * linear) * (x * x)))


def places(count, block):
    me = lax.axis_index("member")
    return [pl.multiple_of((me ^ k) * block, block) for k in range(count)]


def stacked(pieces, cols=slice(None)):
    return jnp.concatenate([piece[:, cols] for piece in pieces], axis=0)


def matched(rows, pieces):
    block = pieces[0].shape[0]
    return jnp.concatenate(
        [rows[:, pl.ds(at, block)] for at in places(len(pieces), block)], axis=1
    )


def norm_matched(source, gain, target, pieces, span=None):
    block = pieces[0].shape[0]
    me = lax.axis_index("member")
    step = 128
    for r in range(*(span or (0, target.shape[0])), step):
        normed = norm_rows(source[r : r + step, :], gain[...])
        for k in range(len(pieces)):
            target[r : r + step, pl.ds(pl.multiple_of((me ^ k) * block, block), block)] = normed[
                :, k * block : (k + 1) * block
            ]


def norm_project(source, gain, normed, pieces, queries, keys, values, third, tile_rows):
    count, width = normed.shape
    step = count // 2
    for r in range(0, count, step):
        norm_matched(source, gain, normed, pieces, (r, r + step))
        at = pl.ds(r, step)
        rows = normed[at, :]
        if queries is not None:
            queries[at, :] = dot(rows, stacked(pieces, slice(0, width))).astype(BF16)
        keys[pl.ds(third * count + r, step), :] = dot(
            rows, stacked(pieces, slice(width, 2 * width))
        ).astype(BF16)
        block = dot(rows, stacked(pieces, slice(2 * width, 3 * width))).astype(BF16)
        for t in range(step // tile_rows):
            slot = (third * count + r) // tile_rows + t
            values[slot] = block[t * tile_rows : (t + 1) * tile_rows].T


def attend_tiles(plan, q_ref, k_ref, v_ref, out_ref, scores, tops, sums, totals, tile_rows, entries):
    rows, width = q_ref.shape
    tiles = rows // tile_rows
    head = width // HEADS
    scale = math.log2(math.e) / math.sqrt(head)
    zero = jnp.zeros((tile_rows, head), BF16)

    def stage(t, p, at):
        row = pl.multiple_of(t * tile_rows, tile_rows)
        first = q_ref[pl.ds(row, tile_rows), 2 * p * head : (2 * p + 1) * head]
        second = q_ref[pl.ds(row, tile_rows), (2 * p + 1) * head : (2 * p + 2) * head]
        both = jnp.concatenate(
            [jnp.concatenate([first, zero], 1), jnp.concatenate([zero, second], 1)], 0
        )
        cols = slice(2 * p * head, (2 * p + 2) * head)
        keys = jnp.concatenate(
            [
                k_ref[pl.ds(pl.multiple_of(plan[t, j] * tile_rows, tile_rows), tile_rows), cols]
                for j in range(entries)
            ],
            0,
        )
        product = dot_t(keys, both)
        scores[at] = product
        top = None
        for j in range(entries):
            part = product[j * tile_rows : (j + 1) * tile_rows]
            part = jnp.max(part.reshape(tile_rows // 8, 8, 2 * tile_rows), axis=0)
            if j >= SURE:
                part = jnp.where(j < plan[8, t], part, -jnp.inf)
            top = part if top is None else jnp.maximum(top, part)
        tops[at] = top

    def blend(t, p, at):
        top = jnp.max(tops[at], axis=0, keepdims=True)
        total, outs = None, [None, None]
        for pair in range(0, entries, 2):
            weights = []
            for j in (pair, pair + 1):
                highest = jnp.where(j < plan[8, t], top, jnp.inf) if j >= SURE else top
                below = scores[at, j * tile_rows : (j + 1) * tile_rows] - highest
                weight = jnp.exp2(below * scale)
                part = jnp.sum(weight.reshape(tile_rows // 8, 8, 2 * tile_rows), axis=0)
                total = part if total is None else total + part
                weights.append(weight.astype(BF16))
            weights = jnp.concatenate(weights, 0)
            for a in range(2):
                h = 2 * p + a
                values = jnp.concatenate(
                    [v_ref[plan[t, j], h * head : (h + 1) * head, :] for j in (pair, pair + 1)], 1
                )
                out = dot(values, weights[:, a * tile_rows : (a + 1) * tile_rows])
                outs[a] = out if outs[a] is None else outs[a] + out
        totals[at] = total
        for a in range(2):
            sums[at, a * head : (a + 1) * head] = outs[a]

    def finish(t, p, at):
        row = pl.multiple_of(t * tile_rows, tile_rows)
        share = 1.0 / jnp.sum(totals[at], axis=0, keepdims=True)
        for a in range(2):
            h = 2 * p + a
            out = sums[at, a * head : (a + 1) * head] * share[:, a * tile_rows : (a + 1) * tile_rows]
            out_ref[pl.ds(row, tile_rows), h * head : (h + 1) * head] = out.T.astype(BF16)

    pairs = HEADS // 2
    totals[...] = jnp.ones(totals.shape, F32)
    sums[...] = jnp.zeros(sums.shape, F32)
    stage(0, 0, 0)

    def one_tile(t, carry):
        for p in range(pairs):
            last = p == pairs - 1
            following = jnp.minimum(t + 1, tiles - 1) if last else t
            stage(following, 0 if last else p + 1, (p + 1) % 2)
            blend(t, p, p % 2)
            before = jnp.maximum(t - 1, 0) if p == 0 else t
            finish(before, (p - 1) % pairs, (p + 1) % 2)
        return carry

    lax.fori_loop(0, tiles, one_tile, 0, unroll=2 if tiles % 2 == 0 else 1)
    finish(tiles - 1, pairs - 1, (pairs - 1) % 2)


def slot_rows(lists, counts, place, ring, own_block):
    tiles, _ = lists.shape
    ids = lists[...]
    other = place ^ 1
    third = lax.rem(place + jnp.where(place & 1 == 1, 1, ring - 1), jnp.int32(ring))

    def inside(device):
        inner = ids - device * tiles
        return (inner >= 0) & (inner < tiles), inner

    mine, inner = inside(place)
    theirs, inner_theirs = inside(other)
    slots = jnp.where(
        mine,
        inner + own_block * tiles,
        jnp.where(
            theirs, inner_theirs + (1 - own_block) * tiles, ids - third * tiles + 2 * tiles
        ),
    )
    return jnp.clip(slots, 0, 3 * tiles - 1).astype(F32), counts[...].astype(F32)


def write_table(target, slots, counts):
    table = jnp.concatenate(
        [
            jnp.pad(slots, ((0, 8 - slots.shape[0]), (0, 128 - slots.shape[1]))),
            jnp.pad(counts, ((0, 7), (0, 128 - counts.shape[1]))),
        ],
        axis=0,
    )
    target[...] = table.astype(BF16)


def pack_body(
    states, lists_in, counts_in, gains_in, more_gains_in, give, keep, table, sent, gains, more_gains,
    lists, counts, sems, *, ring,
):
    place = lax.axis_index("mesh")
    side = place & 1
    copies = [
        pltpu.make_async_copy(lists_in, lists, sems.at[0]),
        pltpu.make_async_copy(counts_in, counts, sems.at[1]),
        pltpu.make_async_copy(states.at[1 - side], give, sems.at[2]),
        pltpu.make_async_copy(states.at[side], keep, sems.at[3]),
        pltpu.make_async_copy(gains_in, gains, sems.at[4]),
        pltpu.make_async_copy(more_gains_in, more_gains, sems.at[5]),
    ]
    for copy in copies:
        copy.start()
    for copy in copies[:2]:
        copy.wait()
    write_table(table, *slot_rows(lists, counts, place, ring, 0))
    write_table(sent, *slot_rows(lists, counts, place, ring, 1))
    for copy in copies[2:]:
        copy.wait()


def stage_body(source, target, sem):
    copy = pltpu.make_async_copy(source, target, sem)
    copy.start()
    copy.wait()


def near_body(source, gain, *rest, n_pieces, tile_rows):
    pieces, (queries, keys, values, normed) = rest[:n_pieces], rest[n_pieces:]
    norm_project(source, gain, normed, pieces, queries, keys, values, 0, tile_rows)


def reach_body(
    table, far, queries, k_keep, v_keep, k_got, v_got, gain, *rest,
    n_pieces, tile_rows, entries,
):
    pieces, (attended, keys, values, normed, scores, tops, sums, totals, whole, plan, sems) = (
        rest[:n_pieces],
        rest[n_pieces:],
    )
    rows = queries.shape[0]
    tiles = rows // tile_rows
    whole[...] = table[...].astype(F32).astype(jnp.int32)
    copies = [
        pltpu.make_async_copy(whole, plan, sems.at[0]),
        pltpu.make_async_copy(k_keep, keys.at[pl.ds(0, rows)], sems.at[1]),
        pltpu.make_async_copy(v_keep, values.at[pl.ds(0, tiles)], sems.at[2]),
        pltpu.make_async_copy(k_got, keys.at[pl.ds(rows, rows)], sems.at[3]),
        pltpu.make_async_copy(v_got, values.at[pl.ds(tiles, tiles)], sems.at[4]),
    ]
    for copy in copies:
        copy.start()
    norm_project(far, gain, normed, pieces, None, keys, values, 2, tile_rows)
    for copy in copies:
        copy.wait()
    attend_tiles(
        plan, queries, keys, values, attended, scores, tops, sums, totals, tile_rows, entries
    )


def middle_rows(states, attended, outs, middle, span=None):
    for r in range(*(span or (0, attended.shape[0])), 128):
        at = pl.ds(r, 128)
        mid = states[at, :].astype(F32) + dot(matched(attended.at[at], outs), stacked(outs))
        middle[at, :] = mid.astype(BF16)


def widen_chunks(normed, middle, ups, downs, hidden, total, early, aside=()):
    block = downs[0].shape[0]
    step = 256
    starts = places(hidden.shape[1] // block, block)
    aside = list(aside)
    behind = None

    def follow():
        if behind is not None:
            k, i, values = behind
            for h in range(total.shape[0]):
                cols = slice(h * 256, (h + 1) * 256)
                part = dot(values, downs[k][i : i + step, cols])
                base = middle[:, cols].astype(F32) if k == i == 0 else total[h]
                total[h] = base + part

    for k, start in enumerate(starts):
        for i in range(0, block, step):
            cols = pl.ds(pl.multiple_of(start + i, step), step)
            wide = dot(normed[...], stacked(ups, cols))
            follow()
            behind = None
            if aside and k >= early:
                aside.pop(0)()
            values = gelu(wide).astype(BF16)
            hidden[:, cols] = values
            if k < early:
                behind = (k, i, values)
    follow()
    for unit in aside:
        unit()


def widen_body(states, attended, gain, *rest, n_pieces, early):
    outs, ups = (rest[i * n_pieces : (i + 1) * n_pieces] for i in range(2))
    downs = rest[2 * n_pieces : 2 * n_pieces + early]
    hidden, total, middle, normed = rest[2 * n_pieces + early :]
    middle_rows(states, attended, outs, middle)
    norm_matched(middle, gain, normed, ups)
    widen_chunks(normed, middle, ups, downs, hidden, total, early)


def rest_body(states, attended, gain, hidden_k, total_in, *rest, n_pieces, early):
    outs, ups = (rest[i * n_pieces : (i + 1) * n_pieces] for i in range(2))
    downs = rest[2 * n_pieces : 3 * n_pieces - 1]
    hidden, total_k, total_g, middle, normed = rest[3 * n_pieces - 1 :]
    block = downs[0].shape[0]
    starts = places(n_pieces, block)

    def unit(k, h):
        def run():
            part = dot(hidden_k[:, pl.ds(starts[k], block)], downs[k][:, h * 256 : (h + 1) * 256])
            total_k[h] = part + (total_in[h] if k == early else total_k[h])

        return run

    units = [unit(k, h) for k in range(early, n_pieces - 1) for h in range(total_k.shape[0])]
    for r in range(0, middle.shape[0], 128):
        middle_rows(states, attended, outs, middle, (r, r + 128))
        if r % 256 == 0 and units:
            units.pop(0)()
        norm_matched(middle, gain, normed, ups, (r, r + 128))
    widen_chunks(normed, middle, ups, downs, hidden, total_g, early, units)


def last_body(total_k, total_g, hidden_k, hidden_g, *rest, n_pieces, early):
    late = n_pieces - early
    downs, (out, staged, sems) = rest[:late], rest[late:]
    side = lax.axis_index("mesh") & 1
    rows, _ = staged.shape[1:]
    block = downs[0].shape[0]
    starts = places(n_pieces, block)[early:]
    copies = []
    step = 256
    for i, (total, hidden, member, first) in enumerate(
        ((total_k, hidden_k, side, late - 1), (total_g, hidden_g, 1 - side, 0))
    ):
        for r in range(0, rows, step):
            at = pl.ds(r, step)
            final = None
            for start, piece in list(zip(starts, downs))[first:]:
                part = dot(hidden[at, pl.ds(start, block)], piece[...])
                final = part if final is None else final + part
            for h in range(total.shape[0]):
                cols = slice(h * 256, (h + 1) * 256)
                staged[i, at, cols] = (total[h, at] + final[:, cols]).astype(BF16)
            copies.append(
                pltpu.make_async_copy(staged.at[i, at], out.at[member, at], sems.at[len(copies)])
            )
            copies[-1].start()
    for copy in copies:
        copy.wait()


def call(body, outs, scratch, operands, spaces, flops, space=VMEM, moved=4 << 20, **static):
    return pl.pallas_call(
        functools.partial(body, **static),
        out_shape=[
            jax.ShapeDtypeStruct(
                [d for d in shape if isinstance(d, int)],
                BF16 if isinstance(shape[-1], int) else shape[-1],
            )
            for shape in outs
        ],
        in_specs=[pl.BlockSpec(memory_space=space) for space in spaces],
        out_specs=[pl.BlockSpec(memory_space=space) for _ in outs],
        scratch_shapes=scratch,
        cost_estimate=pl.CostEstimate(
            flops=flops, bytes_accessed=moved, transcendentals=0
        ),
        compiler_params=pltpu.CompilerParams(vmem_limit_bytes=VMEM_LIMIT),
    )(*operands)


VMEM_LIMIT = 24 << 20


def in_hbm(array):
    return pltpu.with_memory_space_constraint(array, HBM)


def send(axis, perm, array):
    return lax.ppermute(array, axis, perm)


def layer(
    node_states, projection, output_weight, up_weight, down_weight,
    attention_gain, feedforward_gain, tile_lists, tile_counts,
):
    members, rows, width = node_states.shape
    tiles, entries = tile_lists.shape
    tile_rows = rows // tiles
    hidden = up_weight.shape[1]
    ring, n = lax.axis_size("mesh"), lax.axis_size("member")
    if members != 2 or ring % 2 or ring < 4 or n & (n - 1) or RIM_T > tiles or tiles > 8:
        raise ValueError("unsupported mesh")
    bits = [1 << b for b in reversed(range(n.bit_length() - 1))]
    swap = [(i, i ^ 1) for i in range(ring)]
    outward = [(i, (i + (2 if i % 2 else -2)) % ring) for i in range(ring)]
    inward = [(i, (i + (-2 if i % 2 else 2)) % ring) for i in range(ring)]

    def gather(shard):
        pieces = {0: shard}
        for bit in bits:
            perm = [(i, i ^ bit) for i in range(n)]
            for k, piece in list(pieces.items()):
                pieces[k ^ bit] = send("member", perm, piece)
        return [pieces[k] for k in range(n)]

    give, keep, table, sent, gain, second = call(
        pack_body,
        [
            (rows, width), (rows, width), (EXTRA, 128), (EXTRA, 128),
            (1, width, F32), (1, width, F32),
        ],
        [
            pltpu.VMEM((tiles, entries), jnp.int32),
            pltpu.VMEM((1, tiles), jnp.int32),
            pltpu.SemaphoreType.DMA((6,)),
        ],
        [
            in_hbm(x)
            for x in (
                node_states, tile_lists, tile_counts.reshape(1, tiles),
                attention_gain.reshape(1, width), feedforward_gain.reshape(1, width),
            )
        ],
        [HBM] * 5,
        1 << 20, moved=0, ring=ring,
    )
    got = send("mesh", swap, give)
    plan = send("mesh", swap, sent)
    proj = gather(projection)
    far_near = send("mesh", outward, keep)
    far_late = send("mesh", inward, got)
    outs = gather(output_weight)
    ups = gather(up_weight)
    downs = gather(down_weight)

    block = pltpu.VMEM((rows, width), BF16)
    window = [
        pltpu.VMEM((3 * rows, width), BF16),
        pltpu.VMEM((3 * tiles, width, tile_rows), BF16),
        block,
        pltpu.VMEM((2, entries * tile_rows, 2 * tile_rows), F32),
        pltpu.VMEM((2, 8, 2 * tile_rows), F32),
        pltpu.VMEM((2, 2 * width // HEADS, tile_rows), F32),
        pltpu.VMEM((2, 8, 2 * tile_rows), F32),
        pltpu.VMEM((EXTRA, 128), jnp.int32),
        pltpu.SMEM((EXTRA, 128), jnp.int32),
        pltpu.SemaphoreType.DMA((5,)),
    ]

    (own,) = call(
        stage_body,
        [projection.shape],
        [pltpu.SemaphoreType.DMA],
        [in_hbm(projection)],
        [HBM],
        1 << 20, moved=0,
    )
    proj = [own, *proj[1:]]

    def near(source):
        return call(
            near_body,
            [(rows, width), (rows, width), (tiles, width, tile_rows)],
            [block],
            [source, gain, *proj],
            [VMEM] * (2 + n),
            2 << 30, n_pieces=n, tile_rows=tile_rows,
        )

    def reach(table, far, queries):
        (attended,) = call(
            reach_body,
            [(rows, width)],
            window,
            [table, far, queries, k_keep, v_keep, k_got, v_got, gain, *proj],
            [VMEM, VMEM, VMEM, ANY, ANY, ANY, ANY, VMEM] + [VMEM] * n,
            4 << 30, n_pieces=n, tile_rows=tile_rows, entries=entries,
        )
        return attended

    q_keep, k_keep, v_keep = near(keep)
    q_got, k_got, v_got = near(got)
    attended_got = reach(plan, far_near, q_got)
    attended_back = send("mesh", swap, attended_got)
    attended_keep = reach(table, far_late, q_keep)
    early = n // 2
    sums = (width // 256, rows, 256, F32)
    hidden_k, total_k = call(
        widen_body,
        [(rows, hidden), sums],
        [block, block],
        [keep, attended_keep, second, *outs, *ups, *downs[:early]],
        [VMEM] * (3 + 2 * n + early),
        3 << 30, n_pieces=n, early=early,
    )
    hidden_g, total_k, total_g = call(
        rest_body,
        [(rows, hidden), sums, sums],
        [block, block],
        [give, attended_back, second, hidden_k, total_k, *outs, *ups, *downs[:-1]],
        [VMEM] * (4 + 3 * n),
        5 << 30, n_pieces=n, early=early,
    )
    (result,) = call(
        last_body,
        [node_states.shape],
        [pltpu.VMEM((2, rows, width), BF16), pltpu.SemaphoreType.DMA((2 * rows // 256,))],
        [total_k, total_g, hidden_k, hidden_g, *downs[early:]],
        [VMEM] * (4 + n - early),
        2 << 30, space=ANY, n_pieces=n, early=early,
    )
    return result


def solution(mesh):
    in_specs = (
        P("member", "mesh", None),
        P("member", None),
        P("member", None),
        P("member", None),
        P("member", None),
        P(),
        P(),
        P("mesh", None),
        P("mesh"),
    )
    return jax.shard_map(
        layer, mesh=mesh, in_specs=in_specs,
        out_specs=P("member", "mesh", None), check_vma=False,
    )
```

```python
import functools
import math

import jax
import jax.numpy as jnp
from jax import lax
from jax.experimental import pallas as pl
from jax.experimental.pallas import tpu as pltpu
from jax.sharding import PartitionSpec as P

HEADS = 4
RIM_T = 4
EXTRA = 16
SURE = 4
BF16 = jnp.bfloat16
F32 = jnp.float32
VMEM = pltpu.VMEM
ANY = pl.ANY
HBM = pltpu.HBM


def norm_rows(rows, gain):
    values = rows.astype(F32)
    center = values - jnp.mean(values, axis=-1, keepdims=True)
    spread = jnp.mean(center * center, axis=-1, keepdims=True)
    return (center * lax.rsqrt(spread + 1e-05) * gain).astype(BF16)


def dot(a, b):
    return lax.dot_general(a, b, (((1,), (0,)), ((), ())), preferred_element_type=F32)


def dot_t(a, b):
    return lax.dot_general(a, b, (((1,), (1,)), ((), ())), preferred_element_type=F32)


def gelu(x):
    linear = math.sqrt(2 / math.pi)
    half = 0.5 * x
    return half + half * jnp.tanh(x * (linear + (0.044715 * linear) * (x * x)))


def places(count, block):
    me = lax.axis_index("member")
    return [pl.multiple_of((me ^ k) * block, block) for k in range(count)]


def stacked(pieces, cols=slice(None)):
    return jnp.concatenate([piece[:, cols] for piece in pieces], axis=0)


def matched(rows, pieces):
    block = pieces[0].shape[0]
    return jnp.concatenate(
        [rows[:, pl.ds(at, block)] for at in places(len(pieces), block)], axis=1
    )


def norm_matched(source, gain, target, pieces, span=None):
    block = pieces[0].shape[0]
    me = lax.axis_index("member")
    step = 128
    for r in range(*(span or (0, target.shape[0])), step):
        normed = norm_rows(source[r : r + step, :], gain[...])
        for k in range(len(pieces)):
            target[r : r + step, pl.ds(pl.multiple_of((me ^ k) * block, block), block)] = normed[
                :, k * block : (k + 1) * block
            ]


def norm_project(source, gain, normed, pieces, queries, keys, values, third, tile_rows):
    count, width = normed.shape
    step = count // 2
    for r in range(0, count, step):
        norm_matched(source, gain, normed, pieces, (r, r + step))
        at = pl.ds(r, step)
        rows = normed[at, :]
        if queries is not None:
            queries[at, :] = dot(rows, stacked(pieces, slice(0, width))).astype(BF16)
        keys[pl.ds(third * count + r, step), :] = dot(
            rows, stacked(pieces, slice(width, 2 * width))
        ).astype(BF16)
        block = dot(rows, stacked(pieces, slice(2 * width, 3 * width))).astype(BF16)
        for t in range(step // tile_rows):
            slot = (third * count + r) // tile_rows + t
            values[slot] = block[t * tile_rows : (t + 1) * tile_rows].T


def attend_tiles(plan, q_ref, k_ref, v_ref, out_ref, scores, tops, sums, totals, tile_rows, entries):
    rows, width = q_ref.shape
    tiles = rows // tile_rows
    head = width // HEADS
    scale = math.log2(math.e) / math.sqrt(head)
    zero = jnp.zeros((tile_rows, head), BF16)

    def stage(t, p, at):
        row = pl.multiple_of(t * tile_rows, tile_rows)
        first = q_ref[pl.ds(row, tile_rows), 2 * p * head : (2 * p + 1) * head]
        second = q_ref[pl.ds(row, tile_rows), (2 * p + 1) * head : (2 * p + 2) * head]
        both = jnp.concatenate(
            [jnp.concatenate([first, zero], 1), jnp.concatenate([zero, second], 1)], 0
        )
        cols = slice(2 * p * head, (2 * p + 2) * head)
        keys = jnp.concatenate(
            [
                k_ref[pl.ds(pl.multiple_of(plan[t, j] * tile_rows, tile_rows), tile_rows), cols]
                for j in range(entries)
            ],
            0,
        )
        product = dot_t(keys, both)
        scores[at] = product
        top = None
        for j in range(entries):
            part = product[j * tile_rows : (j + 1) * tile_rows]
            part = jnp.max(part.reshape(tile_rows // 8, 8, 2 * tile_rows), axis=0)
            if j >= SURE:
                part = jnp.where(j < plan[8, t], part, -jnp.inf)
            top = part if top is None else jnp.maximum(top, part)
        tops[at] = top

    def blend(t, p, at):
        top = jnp.max(tops[at], axis=0, keepdims=True)
        total, outs = None, [None, None]
        for pair in range(0, entries, 2):
            weights = []
            for j in (pair, pair + 1):
                highest = jnp.where(j < plan[8, t], top, jnp.inf) if j >= SURE else top
                below = scores[at, j * tile_rows : (j + 1) * tile_rows] - highest
                weight = jnp.exp2(below * scale)
                part = jnp.sum(weight.reshape(tile_rows // 8, 8, 2 * tile_rows), axis=0)
                total = part if total is None else total + part
                weights.append(weight.astype(BF16))
            weights = jnp.concatenate(weights, 0)
            for a in range(2):
                h = 2 * p + a
                values = jnp.concatenate(
                    [v_ref[plan[t, j], h * head : (h + 1) * head, :] for j in (pair, pair + 1)], 1
                )
                out = dot(values, weights[:, a * tile_rows : (a + 1) * tile_rows])
                outs[a] = out if outs[a] is None else outs[a] + out
        totals[at] = total
        for a in range(2):
            sums[at, a * head : (a + 1) * head] = outs[a]

    def finish(t, p, at):
        row = pl.multiple_of(t * tile_rows, tile_rows)
        share = 1.0 / jnp.sum(totals[at], axis=0, keepdims=True)
        for a in range(2):
            h = 2 * p + a
            out = sums[at, a * head : (a + 1) * head] * share[:, a * tile_rows : (a + 1) * tile_rows]
            out_ref[pl.ds(row, tile_rows), h * head : (h + 1) * head] = out.T.astype(BF16)

    pairs = HEADS // 2
    totals[...] = jnp.ones(totals.shape, F32)
    sums[...] = jnp.zeros(sums.shape, F32)
    stage(0, 0, 0)

    def one_tile(t, carry):
        for p in range(pairs):
            last = p == pairs - 1
            following = jnp.minimum(t + 1, tiles - 1) if last else t
            stage(following, 0 if last else p + 1, (p + 1) % 2)
            blend(t, p, p % 2)
            before = jnp.maximum(t - 1, 0) if p == 0 else t
            finish(before, (p - 1) % pairs, (p + 1) % 2)
        return carry

    lax.fori_loop(0, tiles, one_tile, 0, unroll=2 if tiles % 2 == 0 else 1)
    finish(tiles - 1, pairs - 1, (pairs - 1) % 2)


def slot_rows(lists, counts, place, ring, own_block):
    tiles, _ = lists.shape
    ids = lists[...]
    other = place ^ 1
    third = lax.rem(place + jnp.where(place & 1 == 1, 1, ring - 1), jnp.int32(ring))

    def inside(device):
        inner = ids - device * tiles
        return (inner >= 0) & (inner < tiles), inner

    mine, inner = inside(place)
    theirs, inner_theirs = inside(other)
    slots = jnp.where(
        mine,
        inner + own_block * tiles,
        jnp.where(
            theirs, inner_theirs + (1 - own_block) * tiles, ids - third * tiles + 2 * tiles
        ),
    )
    return jnp.clip(slots, 0, 3 * tiles - 1).astype(F32), counts[...].astype(F32)


def write_table(target, slots, counts):
    table = jnp.concatenate(
        [
            jnp.pad(slots, ((0, 8 - slots.shape[0]), (0, 128 - slots.shape[1]))),
            jnp.pad(counts, ((0, 7), (0, 128 - counts.shape[1]))),
        ],
        axis=0,
    )
    target[...] = table.astype(BF16)


def pack_body(
    states, lists_in, counts_in, gains_in, more_gains_in, give, keep, table, sent, gains, more_gains,
    lists, counts, sems, *, ring,
):
    place = lax.axis_index("mesh")
    side = place & 1
    copies = [
        pltpu.make_async_copy(lists_in, lists, sems.at[0]),
        pltpu.make_async_copy(counts_in, counts, sems.at[1]),
        pltpu.make_async_copy(states.at[1 - side], give, sems.at[2]),
        pltpu.make_async_copy(states.at[side], keep, sems.at[3]),
        pltpu.make_async_copy(gains_in, gains, sems.at[4]),
        pltpu.make_async_copy(more_gains_in, more_gains, sems.at[5]),
    ]
    for copy in copies:
        copy.start()
    for copy in copies[:2]:
        copy.wait()
    write_table(table, *slot_rows(lists, counts, place, ring, 0))
    write_table(sent, *slot_rows(lists, counts, place, ring, 1))
    for copy in copies[2:]:
        copy.wait()


def stage_body(source, target, sem):
    copy = pltpu.make_async_copy(source, target, sem)
    copy.start()
    copy.wait()


def near_body(source, gain, *rest, n_pieces, tile_rows, asks):
    pieces, (first, keys, values, *scratch) = rest[:n_pieces], rest[n_pieces:]
    queries, normed = (first, scratch[0]) if asks else (None, first)
    norm_project(source, gain, normed, pieces, queries, keys, values, 0, tile_rows)


def ask_body(normed, *rest):
    *pieces, queries = rest
    queries[...] = dot(normed[...], stacked(pieces, slice(0, normed.shape[1]))).astype(BF16)


def reach_body(
    table, far, queries, k_keep, v_keep, k_got, v_got, gain, *rest,
    n_pieces, tile_rows, entries,
):
    pieces, (attended, keys, values, normed, scores, tops, sums, totals, whole, plan, sems) = (
        rest[:n_pieces],
        rest[n_pieces:],
    )
    rows = queries.shape[0]
    tiles = rows // tile_rows
    whole[...] = table[...].astype(F32).astype(jnp.int32)
    copies = [
        pltpu.make_async_copy(whole, plan, sems.at[0]),
        pltpu.make_async_copy(k_keep, keys.at[pl.ds(0, rows)], sems.at[1]),
        pltpu.make_async_copy(v_keep, values.at[pl.ds(0, tiles)], sems.at[2]),
        pltpu.make_async_copy(k_got, keys.at[pl.ds(rows, rows)], sems.at[3]),
        pltpu.make_async_copy(v_got, values.at[pl.ds(tiles, tiles)], sems.at[4]),
    ]
    for copy in copies:
        copy.start()
    norm_project(far, gain, normed, pieces, None, keys, values, 2, tile_rows)
    for copy in copies:
        copy.wait()
    attend_tiles(
        plan, queries, keys, values, attended, scores, tops, sums, totals, tile_rows, entries
    )


def middle_rows(states, attended, outs, middle, span=None):
    for r in range(*(span or (0, attended.shape[0])), 128):
        at = pl.ds(r, 128)
        mid = states[at, :].astype(F32) + dot(matched(attended.at[at], outs), stacked(outs))
        middle[at, :] = mid.astype(BF16)


def widen_chunks(normed, middle, ups, downs, hidden, total, early, aside=()):
    block = downs[0].shape[0]
    step = 256
    starts = places(hidden.shape[1] // block, block)
    aside = list(aside)
    behind = None

    def follow():
        if behind is not None:
            k, i, values = behind
            for h in range(total.shape[0]):
                cols = slice(h * 256, (h + 1) * 256)
                part = dot(values, downs[k][i : i + step, cols])
                base = middle[:, cols].astype(F32) if k == i == 0 else total[h]
                total[h] = base + part

    for k, start in enumerate(starts):
        for i in range(0, block, step):
            cols = pl.ds(pl.multiple_of(start + i, step), step)
            wide = dot(normed[...], stacked(ups, cols))
            follow()
            behind = None
            if aside and k >= early:
                aside.pop(0)()
            values = gelu(wide).astype(BF16)
            hidden[:, cols] = values
            if k < early:
                behind = (k, i, values)
    follow()
    for unit in aside:
        unit()


def widen_body(states, attended, gain, *rest, n_pieces, early):
    outs, ups = (rest[i * n_pieces : (i + 1) * n_pieces] for i in range(2))
    downs = rest[2 * n_pieces : 2 * n_pieces + early]
    hidden, total, middle, normed = rest[2 * n_pieces + early :]
    middle_rows(states, attended, outs, middle)
    norm_matched(middle, gain, normed, ups)
    widen_chunks(normed, middle, ups, downs, hidden, total, early)


def rest_body(states, attended, gain, hidden_k, total_in, *rest, n_pieces, early):
    outs, ups = (rest[i * n_pieces : (i + 1) * n_pieces] for i in range(2))
    downs = rest[2 * n_pieces : 3 * n_pieces - 1]
    hidden, total_k, total_g, middle, normed = rest[3 * n_pieces - 1 :]
    block = downs[0].shape[0]
    starts = places(n_pieces, block)

    def unit(k, h):
        def run():
            part = dot(hidden_k[:, pl.ds(starts[k], block)], downs[k][:, h * 256 : (h + 1) * 256])
            total_k[h] = part + (total_in[h] if k == early else total_k[h])

        return run

    units = [unit(k, h) for k in range(early, n_pieces - 1) for h in range(total_k.shape[0])]
    for r in range(0, middle.shape[0], 128):
        middle_rows(states, attended, outs, middle, (r, r + 128))
        if r % 256 == 0 and units:
            units.pop(0)()
        norm_matched(middle, gain, normed, ups, (r, r + 128))
    widen_chunks(normed, middle, ups, downs, hidden, total_g, early, units)


def last_body(total_k, total_g, hidden_k, hidden_g, *rest, n_pieces, early):
    late = n_pieces - early
    downs, (out, staged, sems) = rest[:late], rest[late:]
    side = lax.axis_index("mesh") & 1
    rows, _ = staged.shape[1:]
    block = downs[0].shape[0]
    starts = places(n_pieces, block)[early:]
    copies = []
    step = 256
    for i, (total, hidden, member, first) in enumerate(
        ((total_k, hidden_k, side, late - 1), (total_g, hidden_g, 1 - side, 0))
    ):
        for r in range(0, rows, step):
            at = pl.ds(r, step)
            final = None
            for start, piece in list(zip(starts, downs))[first:]:
                part = dot(hidden[at, pl.ds(start, block)], piece[...])
                final = part if final is None else final + part
            for h in range(total.shape[0]):
                cols = slice(h * 256, (h + 1) * 256)
                staged[i, at, cols] = (total[h, at] + final[:, cols]).astype(BF16)
            copies.append(
                pltpu.make_async_copy(staged.at[i, at], out.at[member, at], sems.at[len(copies)])
            )
            copies[-1].start()
    for copy in copies:
        copy.wait()


def call(body, outs, scratch, operands, spaces, flops, space=VMEM, moved=4 << 20, **static):
    return pl.pallas_call(
        functools.partial(body, **static),
        out_shape=[
            jax.ShapeDtypeStruct(
                [d for d in shape if isinstance(d, int)],
                BF16 if isinstance(shape[-1], int) else shape[-1],
            )
            for shape in outs
        ],
        in_specs=[pl.BlockSpec(memory_space=space) for space in spaces],
        out_specs=[pl.BlockSpec(memory_space=space) for _ in outs],
        scratch_shapes=scratch,
        cost_estimate=pl.CostEstimate(
            flops=flops, bytes_accessed=moved, transcendentals=0
        ),
        compiler_params=pltpu.CompilerParams(vmem_limit_bytes=VMEM_LIMIT),
    )(*operands)


VMEM_LIMIT = 24 << 20


def in_hbm(array):
    return pltpu.with_memory_space_constraint(array, HBM)


def send(axis, perm, array):
    return lax.ppermute(array, axis, perm)


def layer(
    node_states, projection, output_weight, up_weight, down_weight,
    attention_gain, feedforward_gain, tile_lists, tile_counts,
):
    members, rows, width = node_states.shape
    tiles, entries = tile_lists.shape
    tile_rows = rows // tiles
    hidden = up_weight.shape[1]
    ring, n = lax.axis_size("mesh"), lax.axis_size("member")
    if members != 2 or ring % 2 or ring < 4 or n & (n - 1) or RIM_T > tiles or tiles > 8:
        raise ValueError("unsupported mesh")
    bits = [1 << b for b in reversed(range(n.bit_length() - 1))]
    swap = [(i, i ^ 1) for i in range(ring)]
    outward = [(i, (i + (2 if i % 2 else -2)) % ring) for i in range(ring)]
    inward = [(i, (i + (-2 if i % 2 else 2)) % ring) for i in range(ring)]

    def gather(shard):
        pieces = {0: shard}
        for bit in bits:
            perm = [(i, i ^ bit) for i in range(n)]
            for k, piece in list(pieces.items()):
                pieces[k ^ bit] = send("member", perm, piece)
        return [pieces[k] for k in range(n)]

    give, keep, table, sent, gain, second = call(
        pack_body,
        [
            (rows, width), (rows, width), (EXTRA, 128), (EXTRA, 128),
            (1, width, F32), (1, width, F32),
        ],
        [
            pltpu.VMEM((tiles, entries), jnp.int32),
            pltpu.VMEM((1, tiles), jnp.int32),
            pltpu.SemaphoreType.DMA((6,)),
        ],
        [
            in_hbm(x)
            for x in (
                node_states, tile_lists, tile_counts.reshape(1, tiles),
                attention_gain.reshape(1, width), feedforward_gain.reshape(1, width),
            )
        ],
        [HBM] * 5,
        1 << 20, moved=0, ring=ring,
    )
    got = send("mesh", swap, give)
    plan = send("mesh", swap, sent)
    proj = gather(projection)
    far_near = send("mesh", outward, keep)
    far_late = send("mesh", inward, got)
    outs = gather(output_weight)
    ups = gather(up_weight)
    downs = gather(down_weight)

    block = pltpu.VMEM((rows, width), BF16)
    window = [
        pltpu.VMEM((3 * rows, width), BF16),
        pltpu.VMEM((3 * tiles, width, tile_rows), BF16),
        block,
        pltpu.VMEM((2, entries * tile_rows, 2 * tile_rows), F32),
        pltpu.VMEM((2, 8, 2 * tile_rows), F32),
        pltpu.VMEM((2, 2 * width // HEADS, tile_rows), F32),
        pltpu.VMEM((2, 8, 2 * tile_rows), F32),
        pltpu.VMEM((EXTRA, 128), jnp.int32),
        pltpu.SMEM((EXTRA, 128), jnp.int32),
        pltpu.SemaphoreType.DMA((5,)),
    ]

    (own,) = call(
        stage_body,
        [projection.shape],
        [pltpu.SemaphoreType.DMA],
        [in_hbm(projection)],
        [HBM],
        1 << 20, moved=0,
    )
    proj = [own, *proj[1:]]

    def near(source, asks):
        return call(
            near_body,
            [(rows, width), (rows, width), (tiles, width, tile_rows)],
            [block] if asks else [],
            [source, gain, *proj],
            [VMEM] * (2 + n),
            2 << 30, n_pieces=n, tile_rows=tile_rows, asks=asks,
        )

    def reach(table, far, queries):
        (attended,) = call(
            reach_body,
            [(rows, width)],
            window,
            [table, far, queries, k_keep, v_keep, k_got, v_got, gain, *proj],
            [VMEM, VMEM, VMEM, ANY, ANY, ANY, ANY, VMEM] + [VMEM] * n,
            4 << 30, n_pieces=n, tile_rows=tile_rows, entries=entries,
        )
        return attended

    normed_keep, k_keep, v_keep = near(keep, False)
    q_got, k_got, v_got = near(got, True)
    attended_got = reach(plan, far_near, q_got)
    attended_back = send("mesh", swap, attended_got)
    (q_keep,) = call(ask_body, [(rows, width)], [], [normed_keep, *proj], [VMEM] * (1 + n), 1 << 29)
    attended_keep = reach(table, far_late, q_keep)
    early = n // 2
    sums = (width // 256, rows, 256, F32)
    hidden_k, total_k = call(
        widen_body,
        [(rows, hidden), sums],
        [block, block],
        [keep, attended_keep, second, *outs, *ups, *downs[:early]],
        [VMEM] * (3 + 2 * n + early),
        3 << 30, n_pieces=n, early=early,
    )
    hidden_g, total_k, total_g = call(
        rest_body,
        [(rows, hidden), sums, sums],
        [block, block],
        [give, attended_back, second, hidden_k, total_k, *outs, *ups, *downs[:-1]],
        [VMEM] * (4 + 3 * n),
        5 << 30, n_pieces=n, early=early,
    )
    (result,) = call(
        last_body,
        [node_states.shape],
        [pltpu.VMEM((2, rows, width), BF16), pltpu.SemaphoreType.DMA((2 * rows // 256,))],
        [total_k, total_g, hidden_k, hidden_g, *downs[early:]],
        [VMEM] * (4 + n - early),
        2 << 30, space=ANY, n_pieces=n, early=early,
    )
    return result


def solution(mesh):
    in_specs = (
        P("member", "mesh", None),
        P("member", None),
        P("member", None),
        P("member", None),
        P("member", None),
        P(),
        P(),
        P("mesh", None),
        P("mesh"),
    )
    return jax.shard_map(
        layer, mesh=mesh, in_specs=in_specs,
        out_specs=P("member", "mesh", None), check_vma=False,
    )
```
